32 devices in a mesh: mesh: 8 (over z, x), field: 4 (over y, core).
Axes of the slice: x: 2, y: 2, z: 4, core: 2. Of those that a mesh axis runs over, the one named last changes fastest.
Arguments:
- velocity: float32 [3, 32, 1024], P(None, ('mesh', 'field')), may hold values from -4 to 4
- pressure: float32 [32, 1024], P(('mesh', 'field')), may hold values from -128 to 128
- fields: bfloat16 [3, 256, 32, 1024], P(None, 'field', 'mesh'), may hold values from -1.8 to 1.8
- brownian: bfloat16 [3, 256, 32, 1024], P(None, 'field', 'mesh'), may hold values from -4 to 4
Outputs:
- new_fields: bfloat16 [3, 256, 32, 1024], P(None, 'field', 'mesh')
- new_velocity: float32 [3, 32, 1024], P(None, ('mesh', 'field'))
The draws below stay inside these ranges and needn't reach their ends.
All inputs are finite; a program needn't handle non-finite values.
Results may differ from the reference program's by a relative error of at most 0.001.
Values sent between devices are 32-bit elements; how exact they have to be, the bound alone decides.
A program may use at most 64 MiB of HBM per device.

```python
import math
import jax
import jax.numpy as jnp
from jax import lax

NF = 256
NY = 32
NZ = 32
CXF = 1
SWEEPS = 4
PLANE = 1024
NX = 32


def draw_fields(key, part):
    scale_key, value_key = jax.random.split(jax.random.fold_in(key, 7), 2)
    log_scale = jax.random.uniform(scale_key, (3, 1, NX, PLANE), jnp.float32, math.log(0.3), math.log(1.75))
    node_scale = jnp.exp(log_scale)
    values = jax.random.uniform(value_key, (3, NF, NX, PLANE), jnp.float32, -1.0, 1.0)
    return (node_scale * values).astype(jnp.bfloat16)


def block_scale(rng, shape, cuts, low, high):
    def one(dim, shards_of):
        heights = jax.random.uniform(jax.random.fold_in(jax.random.fold_in(rng, 6), dim), (shards_of,), jnp.float32, low / len(cuts), high / len(cuts))
        return jnp.repeat(jnp.exp(heights), shape[dim] // shards_of).reshape((-1,) + (1,) * (len(shape) - dim - 1))

    gain = one(*cuts[0])
    for cut in cuts[1:]:
        gain = gain * one(*cut)
    return gain


def bell_draw(stream_key, shape, width, limit, cuts=(), kind=jnp.bfloat16):
    level = block_scale(stream_key, shape, cuts, -0.22, 0.18) if cuts else 1.0
    values = jax.random.normal(stream_key, shape, jnp.float32) * width * level
    return jnp.minimum(jnp.maximum(values, -limit), limit).astype(kind)


def setup_inputs(seed: int = 0) -> dict:
    arg_keys = jax.random.split(jax.random.key(seed), 5)
    velocity = bell_draw(arg_keys[0], (3, NX, PLANE), 1.0, 4.0, ((1, 32),), jnp.float32)
    pressure = bell_draw(arg_keys[1], (NX, PLANE), 32.0, 128.0, ((0, 32),), jnp.float32)
    fields = draw_fields(jax.random.fold_in(arg_keys[4], 71), 0)
    brownian = bell_draw(arg_keys[3], (3, NF, NX, PLANE), 1.0, 4.0, ((1, 4), (2, 8)))
    return {"velocity": velocity, "pressure": pressure, "fields": fields, "brownian": brownian}


time_step = 0.02
axial_weight = 400.0
transverse_weight = 40.0
weissenberg = 0.5
max_stretch = 50.0
polymer_viscosity = 40.0
noise_scale = (0.02 / 0.5) ** 0.5
diagonal_weight = 1.0 / 0.02 + 2.0 * 400.0 + 4.0 * 40.0
index_table = ((0, 1, 2), (1, 3, 4), (2, 4, 5))
component_pairs = ((0, 0), (0, 1), (0, 2), (1, 1), (1, 2), (2, 2))


def plane_shifts(values):
    extent = values.shape[-1]
    leading = [(0, 0)] * (values.ndim - 1)
    along_y = jnp.pad(values, leading + [(NZ, NZ)])
    along_z = jnp.pad(values, leading + [(1, 1)])
    column = lax.broadcasted_iota(jnp.int32, (extent,), 0) % NZ
    upper_keep = (column < NZ - 1).astype(values.dtype)
    lower_keep = (column > 0).astype(values.dtype)
    return along_y[..., 2 * NZ:], along_y[..., :extent], along_z[..., 2:] * upper_keep, along_z[..., :extent] * lower_keep


def derivatives(padded):
    interior = padded[:, 1:-1]
    y_plus, y_minus, z_plus, z_minus = plane_shifts(interior)
    return ((padded[:, 2:] - padded[:, :-2]) * 0.5, (y_plus - y_minus) * 0.5, (z_plus - z_minus) * 0.5)


def velocity_gradient(padded):
    stacked = jnp.stack(derivatives(padded), axis=1)
    return stacked.reshape(9, stacked.shape[2], stacked.shape[3])


def advance(fields, brownian, gradient):
    current = fields.astype(jnp.float32)
    increments = brownian.astype(jnp.float32)
    length_sq = current[0] * current[0] + current[1] * current[1] + current[2] * current[2]
    spring = 1.0 / (1.0 - length_sq / max_stretch)
    drift_terms = []
    for out_axis in range(3):
        stretch = gradient[3 * out_axis][None] * current[0] + gradient[3 * out_axis + 1][None] * current[1] + gradient[3 * out_axis + 2][None] * current[2]
        drift_terms.append(stretch - spring * current[out_axis] / (2.0 * weissenberg))
    advanced = current + time_step * jnp.stack(drift_terms) + noise_scale * increments
    new_sq = advanced[0] * advanced[0] + advanced[1] * advanced[1] + advanced[2] * advanced[2]
    new_spring = 1.0 / (1.0 - new_sq / max_stretch)
    partial_value = jnp.stack([jnp.sum(new_spring * advanced[left_axis] * advanced[right_axis], axis=0) for left_axis, right_axis in component_pairs])
    return advanced.astype(jnp.bfloat16), partial_value


def to_stress(summed):
    identity = jnp.array([1.0, 0.0, 0.0, 1.0, 0.0, 1.0], dtype=summed.dtype)[:, None, None]
    return (polymer_viscosity / weissenberg) * (summed / NF - identity)


def momentum_source(velocity, padded_pressure, padded_stress):
    pressure_grad = jnp.concatenate(derivatives(padded_pressure), axis=0)
    slopes = derivatives(padded_stress)
    divergence = jnp.stack([slopes[0][index_table[out_axis][0]] + slopes[1][index_table[out_axis][1]] + slopes[2][index_table[out_axis][2]] for out_axis in range(3)])
    return velocity / time_step - pressure_grad + divergence


def fluid_mask(offset, planes, total_planes, extent):
    position = offset + lax.broadcasted_iota(jnp.int32, (planes, extent), 0)
    across = lax.broadcasted_iota(jnp.int32, (planes, extent), 1) // NZ
    blocked = (position >= total_planes // 2) & ((across < NY // 4) | (across >= NY - NY // 4))
    return jnp.where(blocked, 0.0, 1.0).astype(jnp.float32)


def relax_step(padded, source, fluid):
    interior = padded[:, 1:-1]
    y_plus, y_minus, z_plus, z_minus = plane_shifts(interior)
    along_flow = padded[:, 2:] + padded[:, :-2]
    across_flow = y_plus + y_minus + z_plus + z_minus
    return fluid * (source + axial_weight * along_flow + transverse_weight * across_flow) / diagonal_weight


def reference(velocity, pressure, fields, brownian):
    stacked = jnp.concatenate([velocity, pressure[None]], axis=0)
    padded = jnp.pad(stacked, ((0, 0), (1, 1), (0, 0)))
    gradient = velocity_gradient(padded[:3])

    def one_block(number):
        first_plane = (number * CXF).astype(jnp.int32)
        return advance(lax.dynamic_slice_in_dim(fields, first_plane, CXF, 2),
                       lax.dynamic_slice_in_dim(brownian, first_plane, CXF, 2),
                       lax.dynamic_slice_in_dim(gradient, first_plane, CXF, 1))

    advanced, partial_value = lax.map(one_block, jnp.arange(NX // CXF, dtype=jnp.int32))
    new_fields = jnp.moveaxis(advanced, 0, 2).reshape(3, NF, NX, PLANE)
    summed = jnp.moveaxis(partial_value, 0, 1).reshape(6, NX, PLANE)
    stress = to_stress(summed)
    padded_stress = jnp.pad(stress, ((0, 0), (1, 1), (0, 0)))
    source = momentum_source(velocity, padded[3:], padded_stress)
    fluid = fluid_mask(0, NX, NX, PLANE)
    current = velocity
    for repeat in range(SWEEPS):
        current = relax_step(jnp.pad(current, ((0, 0), (1, 1), (0, 0))), source, fluid)
    return new_fields, current
```

```python
import functools

import jax
import jax.numpy as jnp
from jax import lax
from jax.experimental import pallas as pl
from jax.experimental.pallas import tpu as pltpu
from jax.sharding import PartitionSpec as P

NY = 32
NZ = 32
SWEEPS = 4
LANES = 128
CHUNKS = 4
EARLY_CHUNKS = 2
VMEM_LIMIT = 24 * 1024 * 1024

time_step = 0.02
axial_weight = 400.0
transverse_weight = 40.0
weissenberg = 0.5
max_stretch = 50.0
polymer_viscosity = 40.0
noise_scale = (0.02 / 0.5) ** 0.5
diagonal_weight = 1.0 / 0.02 + 2.0 * 400.0 + 4.0 * 40.0
index_table = ((0, 1, 2), (1, 3, 4), (2, 4, 5))
component_pairs = ((0, 0), (0, 1), (0, 2), (1, 1), (1, 2), (2, 2))
diagonal_pairs = (0, 3, 5)


def plane_shifts(x):
    rows = x.shape[0]
    lane = lax.broadcasted_iota(jnp.int32, x.shape, 1)
    row = lax.broadcasted_iota(jnp.int32, x.shape, 0)
    column = lane % NZ
    ahead = pltpu.roll(x, LANES - NZ, 1)
    ahead_next = jnp.where(row == rows - 1, 0.0, pltpu.roll(ahead, rows - 1, 0))
    y_plus = jnp.where(lane >= LANES - NZ, ahead_next, ahead)
    behind = pltpu.roll(x, NZ, 1)
    behind_next = jnp.where(row == 0, 0.0, pltpu.roll(behind, 1, 0))
    y_minus = jnp.where(lane < NZ, behind_next, behind)
    z_plus = jnp.where(column < NZ - 1, pltpu.roll(x, LANES - 1, 1), 0.0)
    z_minus = jnp.where(column > 0, pltpu.roll(x, 1, 1), 0.0)
    return y_plus, y_minus, z_plus, z_minus


def add(left, right):
    if left is None:
        return right
    return left if right is None else left + right


def step_kernel(
    subdomains, groups,
    vel, prs, fld, brn, advanced, out_vel,
    cur, noise, now32, next32, vbuf, pbuf, tx, rx,
    load_sem, flow_sem, vel_send, vel_mates, vel_cross, con_send, con_recv,
):
    rows = vel.shape[1]
    count = fld.shape[1]
    packed = fld.shape[2]
    total = subdomains * groups
    block = min(16, packed)
    chunk = count // CHUNKS
    reach = -(-SWEEPS // groups)
    spread = 2 * reach + 1
    sub = lax.axis_index("mesh")
    own = lax.axis_index("field")
    has_prev = sub > 0
    has_next = sub < subdomains - 1

    def inside(shift):
        return (sub + shift >= 0) & (sub + shift < subdomains)

    flow_loads = [
        pltpu.make_async_copy(vel, vbuf.at[own + 1], flow_sem.at[0]),
        pltpu.make_async_copy(prs, pbuf, flow_sem.at[1]),
    ]
    for copy in flow_loads:
        copy.start()

    barrier = pltpu.get_barrier_semaphore()

    def greet(device):
        pl.semaphore_signal(
            barrier, inc=1, device_id=device, device_id_type=pl.DeviceIdType.MESH
        )

    @pl.when(has_next)
    def _():
        greet((sub + 1, 0))

    @pl.when(has_prev)
    def _():
        greet((sub - 1, groups - 1))

    for r in range(1, groups):
        greet((sub, (own + r) % groups))

    loads = []
    for number in range(CHUNKS):
        part = pl.ds(number * chunk, chunk)
        loads.append((
            pltpu.make_async_copy(fld.at[:, part], cur.at[:, part], load_sem.at[0, number]),
            pltpu.make_async_copy(brn.at[:, part], noise.at[:, part], load_sem.at[1, number]),
        ))
        for copy in loads[-1]:
            copy.start()

    @pl.when(jnp.logical_not(has_prev))
    def _():
        vbuf[0] = jnp.zeros(vbuf.shape[1:], jnp.float32)

    @pl.when(jnp.logical_not(has_next))
    def _():
        vbuf[groups + 1] = jnp.zeros(vbuf.shape[1:], jnp.float32)

    for shift in range(-reach, reach + 1):
        if shift != 0:
            @pl.when(jnp.logical_not(inside(shift)))
            def _(shift=shift):
                rx[pl.ds((reach + shift) * groups, groups)] = jnp.zeros(
                    (groups,) + rx.shape[1:], jnp.float32
                )

    relax = time_step * max_stretch / (2.0 * weissenberg)

    def base_chunk(number):
        for copy in loads[number]:
            copy.wait()

        @pl.loop(number * chunk, (number + 1) * chunk, unroll=2)
        def _(n):
            for start in range(0, packed, block):
                at = pl.ds(start, block)
                now = [cur[c, n, at].astype(jnp.float32) for c in range(3)]
                square = now[0] * now[0] + now[1] * now[1] + now[2] * now[2]
                keep = 1.0 - relax * (1.0 / (max_stretch - square))
                for c in range(3):
                    now32[c, n, at] = now[c]
                    next32[c, n, at] = now[c] * keep + noise_scale * noise[c, n, at].astype(jnp.float32)

    for number in range(EARLY_CHUNKS):
        base_chunk(number)

    for copy in flow_loads:
        copy.wait()
    sends_prev = (own == 0) & has_prev
    sends_next = (own == groups - 1) & has_next
    greetings = groups - 1 + jnp.where(sends_prev, groups, 0) + jnp.where(sends_next, groups, 0)
    pl.semaphore_wait(barrier, greetings)

    def flow_copy(device, slot, recv):
        return pltpu.make_async_remote_copy(
            src_ref=vbuf.at[own + 1], dst_ref=vbuf.at[slot],
            send_sem=vel_send.at[0], recv_sem=recv,
            device_id=device, device_id_type=pl.DeviceIdType.MESH,
        )

    @pl.when(sends_prev)
    def _():
        for f in reversed(range(groups)):
            flow_copy((sub - 1, f), groups + 1, vel_cross.at[1]).start()

    @pl.when(sends_next)
    def _():
        for f in range(groups):
            flow_copy((sub + 1, f), 0, vel_cross.at[0]).start()

    for r in range(1, groups):
        flow_copy((sub, (own + r) % groups), own + 1, vel_mates.at[0]).start()

    for number in range(EARLY_CHUNKS, CHUNKS):
        base_chunk(number)

    factor = polymer_viscosity / weissenberg
    stress = {}

    def plane_fields(q):
        scale = 0.5 * time_step
        g = [None] * 9
        for a in range(3):
            y_plus, y_minus, z_plus, z_minus = plane_shifts(vbuf[q + 1, a])
            g[3 * a] = (vbuf[q + 2, a] - vbuf[q, a]) * scale
            g[3 * a + 1] = (y_plus - y_minus) * scale
            g[3 * a + 2] = (z_plus - z_minus) * scale
        at = pl.ds(q, rows, stride=groups)

        def one_field(n, acc):
            now = [now32[c, n, at] for c in range(3)]
            new = []
            for a in range(3):
                value = next32[a, n, at] + (
                    g[3 * a] * now[0] + g[3 * a + 1] * now[1] + g[3 * a + 2] * now[2]
                )
                next32[a, n, at] = value
                new.append(value)
            square = new[0] * new[0] + new[1] * new[1] + new[2] * new[2]
            inverse = 1.0 / (max_stretch - square)
            pulled = [inverse * value for value in new]
            return tuple(
                total_k + pulled[left] * new[right]
                for total_k, (left, right) in zip(acc, component_pairs)
            )

        zero = jnp.zeros((rows, LANES), jnp.float32)
        acc = lax.fori_loop(0, count, one_field, (zero,) * 6, unroll=2)
        for k in range(6):
            value = acc[k] * (factor * max_stretch / (count * groups))
            stress[q, k] = value - factor / groups if k in diagonal_pairs else value

    pltpu.make_async_copy(
        vbuf.at[pl.ds(0, groups - 1)], vbuf.at[pl.ds(0, groups - 1)], vel_mates.at[0]
    ).wait()
    for q in range(1, groups - 1):
        plane_fields(q)

    @pl.when(has_prev)
    def _():
        pltpu.make_async_copy(vbuf.at[0], vbuf.at[0], vel_cross.at[0]).wait()

    plane_fields(0)

    @pl.when(has_next)
    def _():
        pltpu.make_async_copy(vbuf.at[0], vbuf.at[0], vel_cross.at[1]).wait()

    plane_fields(groups - 1)

    across = (
        lax.broadcasted_iota(jnp.int32, (rows, LANES), 0) * (LANES // NZ)
        + lax.broadcasted_iota(jnp.int32, (rows, LANES), 1) // NZ
    )
    solid = jnp.where((across < NY // 4) | (across >= NY - NY // 4), 1.0, 0.0)
    first, last = -reach * groups, groups - 1 + reach * groups
    fluid = {}
    for d in range(first, last + 1):
        plane = sub * groups + d
        exists = jnp.where((plane >= 0) & (plane < total), 1.0 / diagonal_weight, 0.0)
        narrow = jnp.where(plane >= total // 2, 1.0, 0.0)
        fluid[d] = exists * (1.0 - narrow * solid)

    mine = [jnp.where(own == q, 1.0, 0.0) for q in range(groups)]
    own_vel = [vbuf[own + 1, a] for a in range(3)]
    own_prs = pbuf[...]
    y_plus, y_minus, z_plus, z_minus = plane_shifts(own_prs)
    own_source = [
        own_vel[0] * (1.0 / time_step),
        own_vel[1] * (1.0 / time_step) - 0.5 * (y_plus - y_minus),
        own_vel[2] * (1.0 / time_step) - 0.5 * (z_plus - z_minus),
    ]
    sources = {}
    for d in range(-1, groups + 1):
        along_y = {}
        along_z = {}
        if 0 <= d < groups:
            for k in range(1, 6):
                y_plus, y_minus, z_plus, z_minus = plane_shifts(stress[d, k])
                along_y[k] = y_plus - y_minus
                along_z[k] = z_plus - z_minus
        for a in range(3):
            slope = None
            if 0 <= d + 1 < groups:
                above = stress[d + 1, a]
                if a == 0:
                    above = above - mine[d + 1] * own_prs
                slope = above
            if 0 <= d - 1 < groups:
                below = stress[d - 1, a]
                if a == 0:
                    below = below - mine[d - 1] * own_prs
                slope = -below if slope is None else slope - below
            if 0 <= d < groups:
                slope = slope + along_y[index_table[a][1]] + along_z[index_table[a][2]]
            value = 0.5 * slope
            if 0 <= d < groups:
                value = value + mine[d] * own_source[a]
            sources[d, a] = value

    for a in range(3):
        v = {q: mine[q] * own_vel[a] for q in range(groups)}
        for sweep in range(1, SWEEPS + 1):
            fresh = {}
            for d in range(-sweep, groups + sweep):
                value = sources.get((d, a))
                if d + 1 in v or d - 1 in v:
                    value = add(value, axial_weight * add(v.get(d + 1), v.get(d - 1)))
                if d in v:
                    y_plus, y_minus, z_plus, z_minus = plane_shifts(v[d])
                    value = add(
                        value,
                        transverse_weight * ((y_plus + y_minus) + (z_plus + z_minus)),
                    )
                fresh[d] = fluid[d] * value
            v = fresh
        for d in range(first, last + 1):
            tx[d - first, a] = v[d] if d in v else jnp.zeros((rows, LANES), jnp.float32)

    def share(shift, f):
        return pltpu.make_async_remote_copy(
            src_ref=tx.at[(reach + shift) * groups + f],
            dst_ref=rx.at[(reach - shift) * groups + own],
            send_sem=con_send.at[0], recv_sem=con_recv.at[0],
            device_id=(sub + shift, f), device_id_type=pl.DeviceIdType.MESH,
        )

    for shift in range(-reach, reach + 1):
        if shift != 0:
            @pl.when(inside(shift))
            def _(shift=shift):
                for r in range(groups):
                    share(shift, (own + r) % groups).start()
        else:
            for r in range(1, groups):
                share(0, (own + r) % groups).start()

    here = reach * groups + own
    rx[here] = tx[here]

    @pl.loop(0, count, unroll=2)
    def _(n):
        for c in range(3):
            for start in range(0, packed, block):
                at = pl.ds(start, block)
                advanced[c, n, at] = next32[c, n, at].astype(jnp.bfloat16)

    partners = groups - 1
    for shift in range(-reach, reach + 1):
        if shift != 0:
            partners = partners + jnp.where(inside(shift), groups, 0)
    sent_flow = groups - 1 + jnp.where(sends_prev, groups, 0) + jnp.where(sends_next, groups, 0)

    def wait_planes(number, options, sem):
        for option in options:
            @pl.when(number == option)
            def _(option=option):
                planes = rx.at[pl.ds(0, option)]
                pltpu.make_async_copy(planes, planes, sem).wait()

    flow_options = [groups - 1 + k * groups for k in range(3)]
    share_options = [groups - 1 + k * groups for k in range(spread)]
    wait_planes(sent_flow, flow_options, vel_send.at[0])
    wait_planes(partners, share_options, con_recv.at[0])
    for a in range(3):
        value = rx[0, a]
        for k in range(1, spread * groups):
            value = value + rx[k, a]
        out_vel[a] = value
    wait_planes(partners, share_options, con_send.at[0])


def write_kernel(advanced, velocity, out_fields, out_vel, out_sem):
    copies = [
        pltpu.make_async_copy(velocity, out_vel, out_sem.at[1]),
        pltpu.make_async_copy(advanced, out_fields, out_sem.at[0]),
    ]
    for copy in copies:
        copy.start()
    for copy in copies:
        copy.wait()


def body(subdomains, groups, velocity, pressure, fields, brownian):
    extent = velocity.shape[2]
    count, depth = fields.shape[1], fields.shape[2]
    rows = extent // LANES
    packed = rows * depth
    slots = (2 * (-(-SWEEPS // groups)) + 1) * groups

    def pack(values):
        split = values.reshape(3, count, depth, rows, LANES)
        return split.transpose(0, 1, 3, 2, 4).reshape(3, count, packed, LANES)

    dma = pltpu.SemaphoreType.DMA
    near = pl.BlockSpec(memory_space=pltpu.VMEM)
    between = pl.pallas_call(
        functools.partial(step_kernel, subdomains, groups),
        out_shape=(
            pltpu.VMEM((3, count, packed, LANES), jnp.bfloat16),
            pltpu.VMEM((3, rows, LANES), jnp.float32),
        ),
        in_specs=[pl.BlockSpec(memory_space=pltpu.HBM)] * 4,
        out_specs=(near,) * 2,
        scratch_shapes=[
            pltpu.VMEM((3, count, packed, LANES), jnp.bfloat16),
            pltpu.VMEM((3, count, packed, LANES), jnp.bfloat16),
            pltpu.VMEM((3, count, packed, LANES), jnp.float32),
            pltpu.VMEM((3, count, packed, LANES), jnp.float32),
            pltpu.VMEM((groups + 2, 3, rows, LANES), jnp.float32),
            pltpu.VMEM((rows, LANES), jnp.float32),
            pltpu.VMEM((slots, 3, rows, LANES), jnp.float32),
            pltpu.VMEM((slots, 3, rows, LANES), jnp.float32),
            dma((2, CHUNKS)),
            dma((2,)),
            dma((1,)),
            dma((1,)),
            dma((2,)),
            dma((1,)),
            dma((1,)),
        ],
        compiler_params=pltpu.CompilerParams(
            collective_id=0, has_side_effects=True, vmem_limit_bytes=VMEM_LIMIT
        ),
    )(
        *(
            pltpu.with_memory_space_constraint(values, pltpu.HBM)
            for values in (
                velocity.reshape(3, rows, LANES),
                pressure.reshape(rows, LANES),
                pack(fields),
                pack(brownian),
            )
        )
    )
    new_fields, new_velocity = pl.pallas_call(
        write_kernel,
        out_shape=(
            jax.ShapeDtypeStruct((3, count, packed, LANES), jnp.bfloat16),
            jax.ShapeDtypeStruct((3, rows, LANES), jnp.float32),
        ),
        in_specs=[near] * 2,
        out_specs=(pl.BlockSpec(memory_space=pltpu.HBM),) * 2,
        scratch_shapes=[dma((2,))],
        compiler_params=pltpu.CompilerParams(vmem_limit_bytes=VMEM_LIMIT),
    )(*between)
    unpacked = new_fields.reshape(3, count, rows, depth, LANES).transpose(0, 1, 3, 2, 4)
    return (
        unpacked.reshape(3, count, depth, extent),
        new_velocity.reshape(3, 1, extent),
    )


def solution(mesh):
    placed = (
        P(None, ("mesh", "field"), None),
        P(("mesh", "field"), None),
        P(None, "field", "mesh", None),
        P(None, "field", "mesh", None),
    )
    return jax.shard_map(
        functools.partial(body, mesh.shape["mesh"], mesh.shape["field"]),
        mesh=mesh,
        in_specs=placed,
        out_specs=(P(None, "field", "mesh", None), P(None, ("mesh", "field"), None)),
        check_vma=False,
    )
```

```python
import functools

import jax
import jax.numpy as jnp
from jax import lax
from jax.experimental import pallas as pl
from jax.experimental.pallas import tpu as pltpu
from jax.sharding import PartitionSpec as P

NY = 32
NZ = 32
SWEEPS = 4
LANES = 128
CHUNKS = 4
EARLY_CHUNKS = 0
VMEM_LIMIT = 24 * 1024 * 1024

time_step = 0.02
axial_weight = 400.0
transverse_weight = 40.0
weissenberg = 0.5
max_stretch = 50.0
polymer_viscosity = 40.0
noise_scale = (0.02 / 0.5) ** 0.5
diagonal_weight = 1.0 / 0.02 + 2.0 * 400.0 + 4.0 * 40.0
index_table = ((0, 1, 2), (1, 3, 4), (2, 4, 5))
component_pairs = ((0, 0), (0, 1), (0, 2), (1, 1), (1, 2), (2, 2))
diagonal_pairs = (0, 3, 5)


def plane_shifts(x):
    rows = x.shape[0]
    lane = lax.broadcasted_iota(jnp.int32, x.shape, 1)
    row = lax.broadcasted_iota(jnp.int32, x.shape, 0)
    column = lane % NZ
    ahead = pltpu.roll(x, LANES - NZ, 1)
    ahead_next = jnp.where(row == rows - 1, 0.0, pltpu.roll(ahead, rows - 1, 0))
    y_plus = jnp.where(lane >= LANES - NZ, ahead_next, ahead)
    behind = pltpu.roll(x, NZ, 1)
    behind_next = jnp.where(row == 0, 0.0, pltpu.roll(behind, 1, 0))
    y_minus = jnp.where(lane < NZ, behind_next, behind)
    z_plus = jnp.where(column < NZ - 1, pltpu.roll(x, LANES - 1, 1), 0.0)
    z_minus = jnp.where(column > 0, pltpu.roll(x, 1, 1), 0.0)
    return y_plus, y_minus, z_plus, z_minus


def add(left, right):
    if left is None:
        return right
    return left if right is None else left + right


def step_kernel(
    subdomains, groups,
    vel, prs, fld, brn, advanced, out_vel,
    cur, noise, now32, next32, vbuf, pbuf, tx, rx,
    load_sem, flow_sem, vel_send, vel_mates, vel_cross, con_send, con_recv,
):
    rows = vel.shape[1]
    count = fld.shape[1]
    packed = fld.shape[2]
    total = subdomains * groups
    block = min(16, packed)
    chunk = count // CHUNKS
    reach = -(-SWEEPS // groups)
    spread = 2 * reach + 1
    sub = lax.axis_index("mesh")
    own = lax.axis_index("field")
    has_prev = sub > 0
    has_next = sub < subdomains - 1

    def inside(shift):
        return (sub + shift >= 0) & (sub + shift < subdomains)

    flow_loads = [
        pltpu.make_async_copy(vel, vbuf.at[own + 1], flow_sem.at[0]),
        pltpu.make_async_copy(prs, pbuf, flow_sem.at[1]),
    ]
    for copy in flow_loads:
        copy.start()

    barrier = pltpu.get_barrier_semaphore()

    def greet(device):
        pl.semaphore_signal(
            barrier, inc=1, device_id=device, device_id_type=pl.DeviceIdType.MESH
        )

    @pl.when(has_next)
    def _():
        greet((sub + 1, 0))

    @pl.when(has_prev)
    def _():
        greet((sub - 1, groups - 1))

    for r in range(1, groups):
        greet((sub, (own + r) % groups))

    loads = []
    for number in range(CHUNKS):
        part = pl.ds(number * chunk, chunk)
        loads.append((
            pltpu.make_async_copy(fld.at[:, part], cur.at[:, part], load_sem.at[0, number]),
            pltpu.make_async_copy(brn.at[:, part], noise.at[:, part], load_sem.at[1, number]),
        ))
        for copy in loads[-1]:
            copy.start()

    @pl.when(jnp.logical_not(has_prev))
    def _():
        vbuf[0] = jnp.zeros(vbuf.shape[1:], jnp.float32)

    @pl.when(jnp.logical_not(has_next))
    def _():
        vbuf[groups + 1] = jnp.zeros(vbuf.shape[1:], jnp.float32)

    for shift in range(-reach, reach + 1):
        if shift != 0:
            @pl.when(jnp.logical_not(inside(shift)))
            def _(shift=shift):
                rx[pl.ds((reach + shift) * groups, groups)] = jnp.zeros(
                    (groups,) + rx.shape[1:], jnp.float32
                )

    relax = time_step * max_stretch / (2.0 * weissenberg)

    def base_chunk(number):
        for copy in loads[number]:
            copy.wait()

        @pl.loop(number * chunk, (number + 1) * chunk, unroll=2)
        def _(n):
            for start in range(0, packed, block):
                at = pl.ds(start, block)
                now = [cur[c, n, at].astype(jnp.float32) for c in range(3)]
                square = now[0] * now[0] + now[1] * now[1] + now[2] * now[2]
                keep = 1.0 - relax * (1.0 / (max_stretch - square))
                for c in range(3):
                    now32[c, n, at] = now[c]
                    next32[c, n, at] = now[c] * keep + noise_scale * noise[c, n, at].astype(jnp.float32)

    for number in range(EARLY_CHUNKS):
        base_chunk(number)

    for copy in flow_loads:
        copy.wait()
    sends_prev = (own == 0) & has_prev
    sends_next = (own == groups - 1) & has_next
    greetings = groups - 1 + jnp.where(sends_prev, groups, 0) + jnp.where(sends_next, groups, 0)
    pl.semaphore_wait(barrier, greetings)

    def flow_copy(device, slot, recv):
        return pltpu.make_async_remote_copy(
            src_ref=vbuf.at[own + 1], dst_ref=vbuf.at[slot],
            send_sem=vel_send.at[0], recv_sem=recv,
            device_id=device, device_id_type=pl.DeviceIdType.MESH,
        )

    @pl.when(sends_prev)
    def _():
        for f in reversed(range(groups)):
            flow_copy((sub - 1, f), groups + 1, vel_cross.at[1]).start()

    @pl.when(sends_next)
    def _():
        for f in range(groups):
            flow_copy((sub + 1, f), 0, vel_cross.at[0]).start()

    for r in range(1, groups):
        flow_copy((sub, (own + r) % groups), own + 1, vel_mates.at[0]).start()

    for number in range(EARLY_CHUNKS, CHUNKS):
        base_chunk(number)

    factor = polymer_viscosity / weissenberg
    stress = {}

    def plane_fields(q):
        scale = 0.5 * time_step
        g = [None] * 9
        for a in range(3):
            y_plus, y_minus, z_plus, z_minus = plane_shifts(vbuf[q + 1, a])
            g[3 * a] = (vbuf[q + 2, a] - vbuf[q, a]) * scale
            g[3 * a + 1] = (y_plus - y_minus) * scale
            g[3 * a + 2] = (z_plus - z_minus) * scale
        at = pl.ds(q, rows, stride=groups)

        def one_field(n, acc):
            now = [now32[c, n, at] for c in range(3)]
            new = []
            for a in range(3):
                value = next32[a, n, at] + (
                    g[3 * a] * now[0] + g[3 * a + 1] * now[1] + g[3 * a + 2] * now[2]
                )
                next32[a, n, at] = value
                new.append(value)
            square = new[0] * new[0] + new[1] * new[1] + new[2] * new[2]
            inverse = 1.0 / (max_stretch - square)
            pulled = [inverse * value for value in new]
            return tuple(
                total_k + pulled[left] * new[right]
                for total_k, (left, right) in zip(acc, component_pairs)
            )

        zero = jnp.zeros((rows, LANES), jnp.float32)
        acc = lax.fori_loop(0, count, one_field, (zero,) * 6, unroll=8)
        for k in range(6):
            value = acc[k] * (factor * max_stretch / (count * groups))
            stress[q, k] = value - factor / groups if k in diagonal_pairs else value

    pltpu.make_async_copy(
        vbuf.at[pl.ds(0, groups - 1)], vbuf.at[pl.ds(0, groups - 1)], vel_mates.at[0]
    ).wait()
    for q in range(1, groups - 1):
        plane_fields(q)

    @pl.when(has_prev)
    def _():
        pltpu.make_async_copy(vbuf.at[0], vbuf.at[0], vel_cross.at[0]).wait()

    plane_fields(0)

    @pl.when(has_next)
    def _():
        pltpu.make_async_copy(vbuf.at[0], vbuf.at[0], vel_cross.at[1]).wait()

    plane_fields(groups - 1)

    across = (
        lax.broadcasted_iota(jnp.int32, (rows, LANES), 0) * (LANES // NZ)
        + lax.broadcasted_iota(jnp.int32, (rows, LANES), 1) // NZ
    )
    solid = jnp.where((across < NY // 4) | (across >= NY - NY // 4), 1.0, 0.0)
    first, last = -reach * groups, groups - 1 + reach * groups
    fluid = {}
    for d in range(first, last + 1):
        plane = sub * groups + d
        exists = jnp.where((plane >= 0) & (plane < total), 1.0 / diagonal_weight, 0.0)
        narrow = jnp.where(plane >= total // 2, 1.0, 0.0)
        fluid[d] = exists * (1.0 - narrow * solid)
    pull = {d: value * transverse_weight for d, value in fluid.items()}

    mine = [jnp.where(own == q, 1.0, 0.0) for q in range(groups)]
    own_vel = [vbuf[own + 1, a] for a in range(3)]
    own_prs = pbuf[...]
    y_plus, y_minus, z_plus, z_minus = plane_shifts(own_prs)
    own_source = [
        own_vel[0] * (1.0 / time_step),
        own_vel[1] * (1.0 / time_step) - 0.5 * (y_plus - y_minus),
        own_vel[2] * (1.0 / time_step) - 0.5 * (z_plus - z_minus),
    ]
    sources = {}
    for d in range(-1, groups + 1):
        along_y = {}
        along_z = {}
        if 0 <= d < groups:
            for k in range(1, 6):
                y_plus, y_minus, z_plus, z_minus = plane_shifts(stress[d, k])
                along_y[k] = y_plus - y_minus
                along_z[k] = z_plus - z_minus
        for a in range(3):
            slope = None
            if 0 <= d + 1 < groups:
                above = stress[d + 1, a]
                if a == 0:
                    above = above - mine[d + 1] * own_prs
                slope = above
            if 0 <= d - 1 < groups:
                below = stress[d - 1, a]
                if a == 0:
                    below = below - mine[d - 1] * own_prs
                slope = -below if slope is None else slope - below
            if 0 <= d < groups:
                slope = slope + along_y[index_table[a][1]] + along_z[index_table[a][2]]
            value = 0.5 * slope
            if 0 <= d < groups:
                value = value + mine[d] * own_source[a]
            sources[d, a] = value

    v = {(q, a): mine[q] * own_vel[a] for q in range(groups) for a in range(3)}
    scaled = {(d, a): fluid[d] * value for (d, a), value in sources.items()}
    ratio = axial_weight / transverse_weight
    for sweep in range(1, SWEEPS + 1):
        fresh = {}
        for d in range(-sweep, groups + sweep):
            for a in range(3):
                value = add(v.get((d + 1, a)), v.get((d - 1, a)))
                if value is not None:
                    value = value * ratio
                if (d, a) in v:
                    y_plus, y_minus, z_plus, z_minus = plane_shifts(v[d, a])
                    value = add(value, (y_plus + y_minus) + (z_plus + z_minus))
                fresh[d, a] = add(scaled.get((d, a)), pull[d] * value)
        v = fresh
    for d in range(first, last + 1):
        for a in range(3):
            tx[d - first, a] = v[d, a] if (d, a) in v else jnp.zeros((rows, LANES), jnp.float32)

    def share(shift, f):
        return pltpu.make_async_remote_copy(
            src_ref=tx.at[(reach + shift) * groups + f],
            dst_ref=rx.at[(reach - shift) * groups + own],
            send_sem=con_send.at[0], recv_sem=con_recv.at[0],
            device_id=(sub + shift, f), device_id_type=pl.DeviceIdType.MESH,
        )

    for shift in range(-reach, reach + 1):
        if shift != 0:
            @pl.when(inside(shift))
            def _(shift=shift):
                for r in range(groups):
                    share(shift, (own + r) % groups).start()
        else:
            for r in range(1, groups):
                share(0, (own + r) % groups).start()

    here = reach * groups + own
    rx[here] = tx[here]

    @pl.loop(0, count, unroll=2)
    def _(n):
        for c in range(3):
            for start in range(0, packed, block):
                at = pl.ds(start, block)
                advanced[c, n, at] = next32[c, n, at].astype(jnp.bfloat16)

    partners = groups - 1
    for shift in range(-reach, reach + 1):
        if shift != 0:
            partners = partners + jnp.where(inside(shift), groups, 0)
    sent_flow = groups - 1 + jnp.where(sends_prev, groups, 0) + jnp.where(sends_next, groups, 0)

    def wait_planes(number, options, sem):
        for option in options:
            @pl.when(number == option)
            def _(option=option):
                planes = rx.at[pl.ds(0, option)]
                pltpu.make_async_copy(planes, planes, sem).wait()

    flow_options = [groups - 1 + k * groups for k in range(3)]
    share_options = [groups - 1 + k * groups for k in range(spread)]
    wait_planes(sent_flow, flow_options, vel_send.at[0])
    wait_planes(partners, share_options, con_recv.at[0])
    for a in range(3):
        value = rx[0, a]
        for k in range(1, spread * groups):
            value = value + rx[k, a]
        out_vel[a] = value
    wait_planes(partners, share_options, con_send.at[0])


def write_kernel(advanced, velocity, out_fields, out_vel, out_sem):
    copies = [
        pltpu.make_async_copy(velocity, out_vel, out_sem.at[1]),
        pltpu.make_async_copy(advanced, out_fields, out_sem.at[0]),
    ]
    for copy in copies:
        copy.start()
    for copy in copies:
        copy.wait()


def body(subdomains, groups, velocity, pressure, fields, brownian):
    extent = velocity.shape[2]
    count, depth = fields.shape[1], fields.shape[2]
    rows = extent // LANES
    packed = rows * depth
    slots = (2 * (-(-SWEEPS // groups)) + 1) * groups

    def pack(values):
        split = values.reshape(3, count, depth, rows, LANES)
        return split.transpose(0, 1, 3, 2, 4).reshape(3, count, packed, LANES)

    dma = pltpu.SemaphoreType.DMA
    near = pl.BlockSpec(memory_space=pltpu.VMEM)
    between = pl.pallas_call(
        functools.partial(step_kernel, subdomains, groups),
        out_shape=(
            pltpu.VMEM((3, count, packed, LANES), jnp.bfloat16),
            pltpu.VMEM((3, rows, LANES), jnp.float32),
        ),
        in_specs=[pl.BlockSpec(memory_space=pltpu.HBM)] * 4,
        out_specs=(near,) * 2,
        scratch_shapes=[
            pltpu.VMEM((3, count, packed, LANES), jnp.bfloat16),
            pltpu.VMEM((3, count, packed, LANES), jnp.bfloat16),
            pltpu.VMEM((3, count, packed, LANES), jnp.float32),
            pltpu.VMEM((3, count, packed, LANES), jnp.float32),
            pltpu.VMEM((groups + 2, 3, rows, LANES), jnp.float32),
            pltpu.VMEM((rows, LANES), jnp.float32),
            pltpu.VMEM((slots, 3, rows, LANES), jnp.float32),
            pltpu.VMEM((slots, 3, rows, LANES), jnp.float32),
            dma((2, CHUNKS)),
            dma((2,)),
            dma((1,)),
            dma((1,)),
            dma((2,)),
            dma((1,)),
            dma((1,)),
        ],
        compiler_params=pltpu.CompilerParams(
            collective_id=0, has_side_effects=True, vmem_limit_bytes=VMEM_LIMIT
        ),
    )(
        *(
            pltpu.with_memory_space_constraint(values, pltpu.HBM)
            for values in (
                velocity.reshape(3, rows, LANES),
                pressure.reshape(rows, LANES),
                pack(fields),
                pack(brownian),
            )
        )
    )
    new_fields, new_velocity = pl.pallas_call(
        write_kernel,
        out_shape=(
            jax.ShapeDtypeStruct((3, count, packed, LANES), jnp.bfloat16),
            jax.ShapeDtypeStruct((3, rows, LANES), jnp.float32),
        ),
        in_specs=[near] * 2,
        out_specs=(pl.BlockSpec(memory_space=pltpu.HBM),) * 2,
        scratch_shapes=[dma((2,))],
        compiler_params=pltpu.CompilerParams(vmem_limit_bytes=VMEM_LIMIT),
    )(*between)
    unpacked = new_fields.reshape(3, count, rows, depth, LANES).transpose(0, 1, 3, 2, 4)
    return (
        unpacked.reshape(3, count, depth, extent),
        new_velocity.reshape(3, 1, extent),
    )


def solution(mesh):
    placed = (
        P(None, ("mesh", "field"), None),
        P(("mesh", "field"), None),
        P(None, "field", "mesh", None),
        P(None, "field", "mesh", None),
    )
    return jax.shard_map(
        functools.partial(body, mesh.shape["mesh"], mesh.shape["field"]),
        mesh=mesh,
        in_specs=placed,
        out_specs=(P(None, "field", "mesh", None), P(None, ("mesh", "field"), None)),
        check_vma=False,
    )
```

```python
import functools

import jax
import jax.numpy as jnp
from jax import lax
from jax.experimental import pallas as pl
from jax.experimental.pallas import tpu as pltpu
from jax.sharding import PartitionSpec as P

NY = 32
NZ = 32
SWEEPS = 4
LANES = 128
CHUNKS = 4
EARLY_CHUNKS = 0
UNROLL = 32
VMEM_LIMIT = 24 * 1024 * 1024

time_step = 0.02
axial_weight = 400.0
transverse_weight = 40.0
weissenberg = 0.5
max_stretch = 50.0
polymer_viscosity = 40.0
noise_scale = (0.02 / 0.5) ** 0.5
diagonal_weight = 1.0 / 0.02 + 2.0 * 400.0 + 4.0 * 40.0
index_table = ((0, 1, 2), (1, 3, 4), (2, 4, 5))
component_pairs = ((0, 0), (0, 1), (0, 2), (1, 1), (1, 2), (2, 2))
diagonal_pairs = (0, 3, 5)


def plane_shifts(x):
    rows = x.shape[0]
    lane = lax.broadcasted_iota(jnp.int32, x.shape, 1)
    row = lax.broadcasted_iota(jnp.int32, x.shape, 0)
    column = lane % NZ
    ahead = pltpu.roll(x, LANES - NZ, 1)
    ahead_next = jnp.where(row == rows - 1, 0.0, pltpu.roll(ahead, rows - 1, 0))
    y_plus = jnp.where(lane >= LANES - NZ, ahead_next, ahead)
    behind = pltpu.roll(x, NZ, 1)
    behind_next = jnp.where(row == 0, 0.0, pltpu.roll(behind, 1, 0))
    y_minus = jnp.where(lane < NZ, behind_next, behind)
    z_plus = jnp.where(column < NZ - 1, pltpu.roll(x, LANES - 1, 1), 0.0)
    z_minus = jnp.where(column > 0, pltpu.roll(x, 1, 1), 0.0)
    return y_plus, y_minus, z_plus, z_minus


def add(left, right):
    if left is None:
        return right
    return left if right is None else left + right


def step_kernel(
    subdomains, groups,
    vel, prs, fld, brn, advanced, out_vel,
    cur, noise, now32, next32, vbuf, pbuf, grads, tx, rx,
    load_sem, flow_sem, vel_send, vel_mates, vel_cross, con_send, con_recv, ready,
):
    rows = vel.shape[1]
    count = fld.shape[1]
    packed = fld.shape[2]
    total = subdomains * groups
    block = min(16, packed)
    chunk = count // CHUNKS
    reach = -(-SWEEPS // groups)
    spread = 2 * reach + 1
    sub = lax.axis_index("mesh")
    own = lax.axis_index("field")
    has_prev = sub > 0
    has_next = sub < subdomains - 1

    def inside(shift):
        return (sub + shift >= 0) & (sub + shift < subdomains)

    flow_loads = [
        pltpu.make_async_copy(vel, vbuf.at[own + 1], flow_sem.at[0]),
        pltpu.make_async_copy(prs, pbuf, flow_sem.at[1]),
    ]
    for copy in flow_loads:
        copy.start()

    barrier = pltpu.get_barrier_semaphore()

    def greet(device):
        pl.semaphore_signal(
            barrier, inc=1, device_id=device, device_id_type=pl.DeviceIdType.MESH
        )

    @pl.when(has_next)
    def _():
        greet((sub + 1, 0))

    @pl.when(has_prev)
    def _():
        greet((sub - 1, groups - 1))

    for helper in range(1, groups - 1):
        @pl.when(own != helper)
        def _(helper=helper):
            greet((sub, helper))

    for number in range(CHUNKS):
        part = pl.ds(number * chunk, chunk)
        for copy in (
            pltpu.make_async_copy(fld.at[:, part], cur.at[:, part], load_sem.at[number]),
            pltpu.make_async_copy(brn.at[:, part], noise.at[:, part], load_sem.at[number]),
        ):
            copy.start()

    @pl.when(jnp.logical_not(has_prev))
    def _():
        vbuf[0] = jnp.zeros(vbuf.shape[1:], jnp.float32)

    @pl.when(jnp.logical_not(has_next))
    def _():
        vbuf[groups + 1] = jnp.zeros(vbuf.shape[1:], jnp.float32)

    for shift in range(-reach, reach + 1):
        if shift != 0:
            @pl.when(jnp.logical_not(inside(shift)))
            def _(shift=shift):
                rx[pl.ds((reach + shift) * groups, groups)] = jnp.zeros(
                    (groups,) + rx.shape[1:], jnp.float32
                )

    relax = time_step * max_stretch / (2.0 * weissenberg)

    def base_chunk(number):
        both = pl.ds(0, 2 * chunk)
        pltpu.make_async_copy(fld.at[:, both], cur.at[:, both], load_sem.at[number]).wait()

        @pl.loop(number * chunk, (number + 1) * chunk, unroll=2)
        def _(n):
            for start in range(0, packed, block):
                at = pl.ds(start, block)
                now = [cur[c, n, at].astype(jnp.float32) for c in range(3)]
                square = now[0] * now[0] + now[1] * now[1] + now[2] * now[2]
                keep = 1.0 - relax * (1.0 / (max_stretch - square))
                for c in range(3):
                    now32[c, n, at] = now[c]
                    next32[c, n, at] = now[c] * keep + noise_scale * noise[c, n, at].astype(jnp.float32)

    for number in range(EARLY_CHUNKS):
        base_chunk(number)

    for copy in flow_loads:
        copy.wait()
    sends_prev = (own == 0) & has_prev
    sends_next = (own == groups - 1) & has_next
    edge = (own == 0) | (own == groups - 1)

    @pl.when(jnp.logical_not(edge))
    def _():
        pl.semaphore_wait(barrier, groups - 1)

    def admit(helper, device):
        @pl.when(own == helper)
        def _():
            pl.semaphore_signal(
                ready, inc=1, device_id=(sub, device), device_id_type=pl.DeviceIdType.MESH
            )

    admit(1, 0)
    admit(groups - 2, groups - 1)

    @pl.when(edge)
    def _():
        pl.semaphore_wait(ready, 1)

    def flow_copy(device, slot, recv):
        return pltpu.make_async_remote_copy(
            src_ref=vbuf.at[own + 1], dst_ref=vbuf.at[slot],
            send_sem=vel_send.at[0], recv_sem=recv,
            device_id=device, device_id_type=pl.DeviceIdType.MESH,
        )

    for r in range(1, groups):
        flow_copy((sub, (own + r) % groups), own + 1, vel_mates.at[0]).start()

    @pl.when(sends_prev)
    def _():
        pl.semaphore_wait(barrier, groups)
        for f in reversed(range(groups)):
            flow_copy((sub - 1, f), groups + 1, vel_cross.at[1]).start()

    @pl.when(sends_next)
    def _():
        pl.semaphore_wait(barrier, groups)
        for f in range(groups):
            flow_copy((sub + 1, f), 0, vel_cross.at[0]).start()

    for number in range(EARLY_CHUNKS, CHUNKS):
        base_chunk(number)

    factor = polymer_viscosity / weissenberg
    stress = {}

    scale = 0.5 * time_step

    def plane_fields(q):
        g = [None] * 9
        for a in range(3):
            g[3 * a] = (vbuf[q + 2, a] - vbuf[q, a]) * scale
            g[3 * a + 1] = grads[q, a]
            g[3 * a + 2] = grads[q, 3 + a]
        at = pl.ds(q, rows, stride=groups)

        def one_field(n, acc):
            now = [now32[c, n, at] for c in range(3)]
            new = []
            for a in range(3):
                value = next32[a, n, at] + (
                    g[3 * a] * now[0] + g[3 * a + 1] * now[1] + g[3 * a + 2] * now[2]
                )
                next32[a, n, at] = value
                new.append(value)
            square = new[0] * new[0] + new[1] * new[1] + new[2] * new[2]
            inverse = 1.0 / (max_stretch - square)
            pulled = [inverse * value for value in new]
            return tuple(
                total_k + pulled[left] * new[right]
                for total_k, (left, right) in zip(acc, component_pairs)
            )

        zero = jnp.zeros((rows, LANES), jnp.float32)
        acc = lax.fori_loop(0, count, one_field, (zero,) * 6, unroll=UNROLL)
        for k in range(6):
            value = acc[k] * (factor * max_stretch / (count * groups))
            stress[q, k] = value - factor / groups if k in diagonal_pairs else value

    pltpu.make_async_copy(
        vbuf.at[pl.ds(0, groups - 1)], vbuf.at[pl.ds(0, groups - 1)], vel_mates.at[0]
    ).wait()
    for q in range(groups):
        for a in range(3):
            y_plus, y_minus, z_plus, z_minus = plane_shifts(vbuf[q + 1, a])
            grads[q, a] = (y_plus - y_minus) * scale
            grads[q, 3 + a] = (z_plus - z_minus) * scale
    for q in range(1, groups - 1):
        plane_fields(q)

    @pl.when(has_prev)
    def _():
        pltpu.make_async_copy(vbuf.at[0], vbuf.at[0], vel_cross.at[0]).wait()

    plane_fields(0)

    @pl.when(has_next)
    def _():
        pltpu.make_async_copy(vbuf.at[0], vbuf.at[0], vel_cross.at[1]).wait()

    plane_fields(groups - 1)

    across = (
        lax.broadcasted_iota(jnp.int32, (rows, LANES), 0) * (LANES // NZ)
        + lax.broadcasted_iota(jnp.int32, (rows, LANES), 1) // NZ
    )
    solid = jnp.where((across < NY // 4) | (across >= NY - NY // 4), 1.0, 0.0)
    first, last = -reach * groups, groups - 1 + reach * groups
    fluid = {}
    for d in range(first, last + 1):
        plane = sub * groups + d
        exists = jnp.where((plane >= 0) & (plane < total), 1.0 / diagonal_weight, 0.0)
        narrow = jnp.where(plane >= total // 2, 1.0, 0.0)
        fluid[d] = exists * (1.0 - narrow * solid)
    pull = {d: value * transverse_weight for d, value in fluid.items()}

    mine = [jnp.where(own == q, 1.0, 0.0) for q in range(groups)]
    own_vel = [vbuf[own + 1, a] for a in range(3)]
    own_prs = pbuf[...]
    y_plus, y_minus, z_plus, z_minus = plane_shifts(own_prs)
    own_source = [
        own_vel[0] * (1.0 / time_step),
        own_vel[1] * (1.0 / time_step) - 0.5 * (y_plus - y_minus),
        own_vel[2] * (1.0 / time_step) - 0.5 * (z_plus - z_minus),
    ]
    sources = {}
    for d in range(-1, groups + 1):
        along_y = {}
        along_z = {}
        if 0 <= d < groups:
            for k in range(1, 6):
                y_plus, y_minus, z_plus, z_minus = plane_shifts(stress[d, k])
                along_y[k] = y_plus - y_minus
                along_z[k] = z_plus - z_minus
        for a in range(3):
            slope = None
            if 0 <= d + 1 < groups:
                above = stress[d + 1, a]
                if a == 0:
                    above = above - mine[d + 1] * own_prs
                slope = above
            if 0 <= d - 1 < groups:
                below = stress[d - 1, a]
                if a == 0:
                    below = below - mine[d - 1] * own_prs
                slope = -below if slope is None else slope - below
            if 0 <= d < groups:
                slope = slope + along_y[index_table[a][1]] + along_z[index_table[a][2]]
            value = 0.5 * slope
            if 0 <= d < groups:
                value = value + mine[d] * own_source[a]
            sources[d, a] = value

    v = {(q, a): mine[q] * own_vel[a] for q in range(groups) for a in range(3)}
    scaled = {(d, a): fluid[d] * value for (d, a), value in sources.items()}
    ratio = axial_weight / transverse_weight
    for sweep in range(1, SWEEPS + 1):
        fresh = {}
        for d in range(-sweep, groups + sweep):
            for a in range(3):
                value = add(v.get((d + 1, a)), v.get((d - 1, a)))
                if value is not None:
                    value = value * ratio
                if (d, a) in v:
                    y_plus, y_minus, z_plus, z_minus = plane_shifts(v[d, a])
                    value = add(value, (y_plus + y_minus) + (z_plus + z_minus))
                fresh[d, a] = add(scaled.get((d, a)), pull[d] * value)
        v = fresh
    for d in range(first, last + 1):
        for a in range(3):
            tx[d - first, a] = v[d, a] if (d, a) in v else jnp.zeros((rows, LANES), jnp.float32)

    def share(shift, f):
        return pltpu.make_async_remote_copy(
            src_ref=tx.at[(reach + shift) * groups + f],
            dst_ref=rx.at[(reach - shift) * groups + own],
            send_sem=con_send.at[0], recv_sem=con_recv.at[0],
            device_id=(sub + shift, f), device_id_type=pl.DeviceIdType.MESH,
        )

    half = max(1, groups // 2)
    across_first = (own // half + 1) * half
    for shift in range(-reach, reach + 1):
        if shift != 0:
            @pl.when(inside(shift))
            def _(shift=shift):
                for r in range(groups):
                    share(shift, (across_first + r) % groups).start()
        else:
            for r in range(1, groups):
                share(0, (own + r) % groups).start()

    here = reach * groups + own
    rx[here] = tx[here]

    @pl.loop(0, count, unroll=2)
    def _(n):
        for c in range(3):
            for start in range(0, packed, block):
                at = pl.ds(start, block)
                advanced[c, n, at] = next32[c, n, at].astype(jnp.bfloat16)

    partners = groups - 1
    for shift in range(-reach, reach + 1):
        if shift != 0:
            partners = partners + jnp.where(inside(shift), groups, 0)
    sent_flow = groups - 1 + jnp.where(sends_prev, groups, 0) + jnp.where(sends_next, groups, 0)

    def wait_planes(number, options, sem):
        for option in options:
            @pl.when(number == option)
            def _(option=option):
                planes = rx.at[pl.ds(0, option)]
                pltpu.make_async_copy(planes, planes, sem).wait()

    flow_options = [groups - 1 + k * groups for k in range(3)]
    share_options = [groups - 1 + k * groups for k in range(spread)]
    wait_planes(sent_flow, flow_options, vel_send.at[0])
    wait_planes(partners, share_options, con_recv.at[0])
    for a in range(3):
        value = rx[0, a]
        for k in range(1, spread * groups):
            value = value + rx[k, a]
        out_vel[a] = value
    wait_planes(partners, share_options, con_send.at[0])


def write_kernel(advanced, velocity, out_fields, out_vel, out_sem):
    copies = [
        pltpu.make_async_copy(velocity, out_vel, out_sem.at[1]),
        pltpu.make_async_copy(advanced, out_fields, out_sem.at[0]),
    ]
    for copy in copies:
        copy.start()
    for copy in copies:
        copy.wait()


def body(subdomains, groups, velocity, pressure, fields, brownian):
    extent = velocity.shape[2]
    count, depth = fields.shape[1], fields.shape[2]
    rows = extent // LANES
    packed = rows * depth
    slots = (2 * (-(-SWEEPS // groups)) + 1) * groups

    def pack(values):
        split = values.reshape(3, count, depth, rows, LANES)
        return split.transpose(0, 1, 3, 2, 4).reshape(3, count, packed, LANES)

    dma = pltpu.SemaphoreType.DMA
    near = pl.BlockSpec(memory_space=pltpu.VMEM)
    between = pl.pallas_call(
        functools.partial(step_kernel, subdomains, groups),
        out_shape=(
            pltpu.VMEM((3, count, packed, LANES), jnp.bfloat16),
            pltpu.VMEM((3, rows, LANES), jnp.float32),
        ),
        in_specs=[pl.BlockSpec(memory_space=pltpu.HBM)] * 4,
        out_specs=(near,) * 2,
        scratch_shapes=[
            pltpu.VMEM((3, count, packed, LANES), jnp.bfloat16),
            pltpu.VMEM((3, count, packed, LANES), jnp.bfloat16),
            pltpu.VMEM((3, count, packed, LANES), jnp.float32),
            pltpu.VMEM((3, count, packed, LANES), jnp.float32),
            pltpu.VMEM((groups + 2, 3, rows, LANES), jnp.float32),
            pltpu.VMEM((rows, LANES), jnp.float32),
            pltpu.VMEM((groups, 6, rows, LANES), jnp.float32),
            pltpu.VMEM((slots, 3, rows, LANES), jnp.float32),
            pltpu.VMEM((slots, 3, rows, LANES), jnp.float32),
            dma((CHUNKS,)),
            dma((2,)),
            dma((1,)),
            dma((1,)),
            dma((2,)),
            dma((1,)),
            dma((1,)),
            pltpu.SemaphoreType.REGULAR,
        ],
        compiler_params=pltpu.CompilerParams(
            collective_id=0, has_side_effects=True, vmem_limit_bytes=VMEM_LIMIT
        ),
    )(
        *(
            pltpu.with_memory_space_constraint(values, pltpu.HBM)
            for values in (
                velocity.reshape(3, rows, LANES),
                pressure.reshape(rows, LANES),
                pack(fields),
                pack(brownian),
            )
        )
    )
    new_fields, new_velocity = pl.pallas_call(
        write_kernel,
        out_shape=(
            jax.ShapeDtypeStruct((3, count, packed, LANES), jnp.bfloat16),
            jax.ShapeDtypeStruct((3, rows, LANES), jnp.float32),
        ),
        in_specs=[near] * 2,
        out_specs=(pl.BlockSpec(memory_space=pltpu.HBM),) * 2,
        scratch_shapes=[dma((2,))],
        compiler_params=pltpu.CompilerParams(vmem_limit_bytes=VMEM_LIMIT),
    )(*between)
    unpacked = new_fields.reshape(3, count, rows, depth, LANES).transpose(0, 1, 3, 2, 4)
    return (
        unpacked.reshape(3, count, depth, extent),
        new_velocity.reshape(3, 1, extent),
    )


def solution(mesh):
    placed = (
        P(None, ("mesh", "field"), None),
        P(("mesh", "field"), None),
        P(None, "field", "mesh", None),
        P(None, "field", "mesh", None),
    )
    return jax.shard_map(
        functools.partial(body, mesh.shape["mesh"], mesh.shape["field"]),
        mesh=mesh,
        in_specs=placed,
        out_specs=(P(None, "field", "mesh", None), P(None, ("mesh", "field"), None)),
        check_vma=False,
    )
```

```python
import functools

import jax
import jax.numpy as jnp
from jax import lax
from jax.experimental import pallas as pl
from jax.experimental.pallas import tpu as pltpu
from jax.sharding import PartitionSpec as P

NY = 32
NZ = 32
SWEEPS = 4
LANES = 128
CHUNKS = 4
EARLY_CHUNKS = 0
UNROLL = 32
VMEM_LIMIT = 24 * 1024 * 1024

time_step = 0.02
axial_weight = 400.0
transverse_weight = 40.0
weissenberg = 0.5
max_stretch = 50.0
polymer_viscosity = 40.0
noise_scale = (0.02 / 0.5) ** 0.5
diagonal_weight = 1.0 / 0.02 + 2.0 * 400.0 + 4.0 * 40.0
index_table = ((0, 1, 2), (1, 3, 4), (2, 4, 5))
component_pairs = ((0, 0), (0, 1), (0, 2), (1, 1), (1, 2), (2, 2))
diagonal_pairs = (0, 3, 5)


def plane_shifts(x):
    rows = x.shape[0]
    lane = lax.broadcasted_iota(jnp.int32, x.shape, 1)
    row = lax.broadcasted_iota(jnp.int32, x.shape, 0)
    column = lane % NZ
    ahead = pltpu.roll(x, LANES - NZ, 1)
    ahead_next = jnp.where(row == rows - 1, 0.0, pltpu.roll(ahead, rows - 1, 0))
    y_plus = jnp.where(lane >= LANES - NZ, ahead_next, ahead)
    behind = pltpu.roll(x, NZ, 1)
    behind_next = jnp.where(row == 0, 0.0, pltpu.roll(behind, 1, 0))
    y_minus = jnp.where(lane < NZ, behind_next, behind)
    z_plus = jnp.where(column < NZ - 1, pltpu.roll(x, LANES - 1, 1), 0.0)
    z_minus = jnp.where(column > 0, pltpu.roll(x, 1, 1), 0.0)
    return y_plus, y_minus, z_plus, z_minus


def add(left, right):
    if left is None:
        return right
    return left if right is None else left + right


def step_kernel(
    subdomains, groups,
    vel, prs, fld, brn, advanced, out_vel,
    cur, noise, now32, next32, vbuf, pbuf, grads, stress, terms, tx, rx,
    load_sem, flow_sem, vel_send, vel_mates, vel_cross, con_send, con_recv, ready,
):
    rows = vel.shape[1]
    count = fld.shape[1]
    packed = fld.shape[2]
    total = subdomains * groups
    block = min(16, packed)
    chunk = count // CHUNKS
    reach = -(-SWEEPS // groups)
    spread = 2 * reach + 1
    sub = lax.axis_index("mesh")
    own = lax.axis_index("field")
    has_prev = sub > 0
    has_next = sub < subdomains - 1

    def inside(shift):
        return (sub + shift >= 0) & (sub + shift < subdomains)

    flow_loads = [
        pltpu.make_async_copy(vel, vbuf.at[own + 1], flow_sem.at[0]),
        pltpu.make_async_copy(prs, pbuf, flow_sem.at[1]),
    ]
    for copy in flow_loads:
        copy.start()

    barrier = pltpu.get_barrier_semaphore()

    def greet(device):
        pl.semaphore_signal(
            barrier, inc=1, device_id=device, device_id_type=pl.DeviceIdType.MESH
        )

    @pl.when(has_next)
    def _():
        greet((sub + 1, 0))

    @pl.when(has_prev)
    def _():
        greet((sub - 1, groups - 1))

    for helper in range(1, groups - 1):
        @pl.when(own != helper)
        def _(helper=helper):
            greet((sub, helper))

    for number in range(CHUNKS):
        part = pl.ds(number * chunk, chunk)
        for copy in (
            pltpu.make_async_copy(fld.at[:, part], cur.at[:, part], load_sem.at[number]),
            pltpu.make_async_copy(brn.at[:, part], noise.at[:, part], load_sem.at[number]),
        ):
            copy.start()

    @pl.when(jnp.logical_not(has_prev))
    def _():
        vbuf[0] = jnp.zeros(vbuf.shape[1:], jnp.float32)

    @pl.when(jnp.logical_not(has_next))
    def _():
        vbuf[groups + 1] = jnp.zeros(vbuf.shape[1:], jnp.float32)

    for shift in range(-reach, reach + 1):
        if shift != 0:
            @pl.when(jnp.logical_not(inside(shift)))
            def _(shift=shift):
                rx[pl.ds((reach + shift) * groups, groups)] = jnp.zeros(
                    (groups,) + rx.shape[1:], jnp.float32
                )

    relax = time_step * max_stretch / (2.0 * weissenberg)

    def base_chunk(number):
        both = pl.ds(0, 2 * chunk)
        pltpu.make_async_copy(fld.at[:, both], cur.at[:, both], load_sem.at[number]).wait()

        @pl.loop(number * chunk, (number + 1) * chunk, unroll=2)
        def _(n):
            for start in range(0, packed, block):
                at = pl.ds(start, block)
                now = [cur[c, n, at].astype(jnp.float32) for c in range(3)]
                square = now[0] * now[0] + now[1] * now[1] + now[2] * now[2]
                keep = 1.0 - relax * (1.0 / (max_stretch - square))
                for c in range(3):
                    now32[c, n, at] = now[c]
                    next32[c, n, at] = now[c] * keep + noise_scale * noise[c, n, at].astype(jnp.float32)

    for number in range(EARLY_CHUNKS):
        base_chunk(number)

    for copy in flow_loads:
        copy.wait()
    sends_prev = (own == 0) & has_prev
    sends_next = (own == groups - 1) & has_next
    edge = (own == 0) | (own == groups - 1)

    @pl.when(jnp.logical_not(edge))
    def _():
        pl.semaphore_wait(barrier, groups - 1)

    def admit(helper, device):
        @pl.when(own == helper)
        def _():
            pl.semaphore_signal(
                ready, inc=1, device_id=(sub, device), device_id_type=pl.DeviceIdType.MESH
            )

    admit(1, 0)
    admit(groups - 2, groups - 1)

    @pl.when(edge)
    def _():
        pl.semaphore_wait(ready, 1)

    def flow_copy(device, slot, recv):
        return pltpu.make_async_remote_copy(
            src_ref=vbuf.at[own + 1], dst_ref=vbuf.at[slot],
            send_sem=vel_send.at[0], recv_sem=recv,
            device_id=device, device_id_type=pl.DeviceIdType.MESH,
        )

    for r in range(1, groups):
        flow_copy((sub, (own + r) % groups), own + 1, vel_mates.at[0]).start()

    @pl.when(sends_prev)
    def _():
        pl.semaphore_wait(barrier, groups)
        for f in sorted(range(groups), key=lambda f: (f % 2, -f)):
            flow_copy((sub - 1, f), groups + 1, vel_cross.at[1]).start()

    @pl.when(sends_next)
    def _():
        pl.semaphore_wait(barrier, groups)
        for f in sorted(range(groups), key=lambda f: (f % 2, f)):
            flow_copy((sub + 1, f), 0, vel_cross.at[0]).start()

    for number in range(EARLY_CHUNKS, CHUNKS):
        base_chunk(number)

    factor = polymer_viscosity / weissenberg

    scale = 0.5 * time_step

    def plane_fields(q):
        g = [None] * 9
        for a in range(3):
            g[3 * a] = (vbuf[q + 2, a] - vbuf[q, a]) * scale
            g[3 * a + 1] = grads[q, a]
            g[3 * a + 2] = grads[q, 3 + a]
        at = pl.ds(q, rows, stride=groups)

        def one_field(n, acc):
            now = [now32[c, n, at] for c in range(3)]
            new = []
            for a in range(3):
                value = next32[a, n, at] + (
                    g[3 * a] * now[0] + g[3 * a + 1] * now[1] + g[3 * a + 2] * now[2]
                )
                next32[a, n, at] = value
                new.append(value)
            square = new[0] * new[0] + new[1] * new[1] + new[2] * new[2]
            inverse = 1.0 / (max_stretch - square)
            pulled = [inverse * value for value in new]
            return tuple(
                total_k + pulled[left] * new[right]
                for total_k, (left, right) in zip(acc, component_pairs)
            )

        zero = jnp.zeros((rows, LANES), jnp.float32)
        acc = lax.fori_loop(0, count, one_field, (zero,) * 6, unroll=UNROLL)
        for k in range(6):
            value = acc[k] * (factor * max_stretch / (count * groups))
            stress[q, k] = value - factor / groups if k in diagonal_pairs else value

    across = (
        lax.broadcasted_iota(jnp.int32, (rows, LANES), 0) * (LANES // NZ)
        + lax.broadcasted_iota(jnp.int32, (rows, LANES), 1) // NZ
    )
    solid = jnp.where((across < NY // 4) | (across >= NY - NY // 4), 1.0, 0.0)
    first, last = -reach * groups, groups - 1 + reach * groups
    mine = [jnp.where(own == q, 1.0, 0.0) for q in range(groups)]
    y_plus, y_minus, z_plus, z_minus = plane_shifts(pbuf[...])
    pressure_slopes = (None, y_plus - y_minus, z_plus - z_minus)
    for a in range(3):
        mid = vbuf[own + 1, a]
        y_plus, y_minus, z_plus, z_minus = plane_shifts(mid)
        terms[a] = transverse_weight * ((y_plus + y_minus) + (z_plus + z_minus))
        value = mid * (1.0 / time_step)
        terms[3 + a] = value if a == 0 else value - 0.5 * pressure_slopes[a]

    def fluid(d):
        plane = sub * groups + d
        exists = jnp.where((plane >= 0) & (plane < total), 1.0 / diagonal_weight, 0.0)
        narrow = jnp.where(plane >= total // 2, 1.0, 0.0)
        return exists * (1.0 - narrow * solid)

    def momentum(outputs):
        needs = {SWEEPS: sorted(outputs)}
        for sweep in range(SWEEPS, 1, -1):
            around = {d + e for d in needs[sweep] for e in (-1, 0, 1)}
            needs[sweep - 1] = sorted(
                d for d in around if -sweep < d < groups + sweep - 1
            )
        scale_of = {}
        source = {}
        start = {}
        for d in sorted({d for ds in needs.values() for d in ds}):
            scale_of[d] = fluid(d)
            if not -1 <= d <= groups:
                continue
            along_y = {}
            along_z = {}
            if 0 <= d < groups:
                for k in range(1, 6):
                    y_plus, y_minus, z_plus, z_minus = plane_shifts(stress[d, k])
                    along_y[k] = y_plus - y_minus
                    along_z[k] = z_plus - z_minus
            for a in range(3):
                slope = None
                beside = 0.0
                for e, sign in ((1, 1.0), (-1, -1.0)):
                    if 0 <= d + e < groups:
                        other = stress[d + e, a]
                        if a == 0:
                            other = other - mine[d + e] * pbuf[...]
                        slope = add(slope, sign * other)
                        beside = beside + mine[d + e]
                if 0 <= d < groups:
                    slope = add(slope, along_y[index_table[a][1]] + along_z[index_table[a][2]])
                value = 0.5 * slope
                begin = (axial_weight * beside) * vbuf[own + 1, a]
                if 0 <= d < groups:
                    value = value + mine[d] * terms[3 + a]
                    begin = begin + mine[d] * terms[a]
                source[d, a] = scale_of[d] * value
                start[d, a] = source[d, a] + scale_of[d] * begin
        pull = {d: value * transverse_weight for d, value in scale_of.items()}
        ratio = axial_weight / transverse_weight
        v = {(d, a): start[d, a] for d in needs[1] for a in range(3)}
        for sweep in range(2, SWEEPS + 1):
            fresh = {}
            for d in needs[sweep]:
                for a in range(3):
                    value = add(v.get((d + 1, a)), v.get((d - 1, a)))
                    if value is not None:
                        value = value * ratio
                    if (d, a) in v:
                        y_plus, y_minus, z_plus, z_minus = plane_shifts(v[d, a])
                        value = add(value, (y_plus + y_minus) + (z_plus + z_minus))
                    fresh[d, a] = add(source.get((d, a)), pull[d] * value)
            v = fresh
        for d in outputs:
            for a in range(3):
                tx[d - first, a] = v[d, a]

    def share(shift, f):
        return pltpu.make_async_remote_copy(
            src_ref=tx.at[(reach + shift) * groups + f],
            dst_ref=rx.at[(reach - shift) * groups + own],
            send_sem=con_send.at[0], recv_sem=con_recv.at[0],
            device_id=(sub + shift, f), device_id_type=pl.DeviceIdType.MESH,
        )

    pltpu.make_async_copy(
        vbuf.at[pl.ds(0, groups - 1)], vbuf.at[pl.ds(0, groups - 1)], vel_mates.at[0]
    ).wait()
    for q in range(groups):
        for a in range(3):
            y_plus, y_minus, z_plus, z_minus = plane_shifts(vbuf[q + 1, a])
            grads[q, a] = (y_plus - y_minus) * scale
            grads[q, 3 + a] = (z_plus - z_minus) * scale
    for q in range(1, groups - 1):
        plane_fields(q)

    @pl.when(has_prev)
    def _():
        pltpu.make_async_copy(vbuf.at[0], vbuf.at[0], vel_cross.at[0]).wait()

    plane_fields(0)

    half = max(1, groups // 2)
    across_first = (own // half + 1) * half
    early = groups - 1 - SWEEPS - first

    @pl.when(has_prev)
    def _():
        momentum(range(first, first + early))
        for r in range(groups):
            f = (across_first + r) % groups

            @pl.when(f < early)
            def _(f=f):
                share(-reach, f).start()

    @pl.when(has_next)
    def _():
        pltpu.make_async_copy(vbuf.at[0], vbuf.at[0], vel_cross.at[1]).wait()

    plane_fields(groups - 1)
    momentum(range(first + early, last + 1))

    @pl.when(has_prev)
    def _():
        for f in range(early, groups):
            share(-reach, f).start()

    @pl.when(has_next)
    def _():
        for r in range(groups):
            share(reach, (across_first + r) % groups).start()

    for r in range(1, groups):
        share(0, (own + r) % groups).start()

    here = reach * groups + own
    rx[here] = tx[here]

    @pl.loop(0, count, unroll=2)
    def _(n):
        for c in range(3):
            for start in range(0, packed, block):
                at = pl.ds(start, block)
                advanced[c, n, at] = next32[c, n, at].astype(jnp.bfloat16)

    partners = groups - 1
    for shift in range(-reach, reach + 1):
        if shift != 0:
            partners = partners + jnp.where(inside(shift), groups, 0)
    sent_flow = groups - 1 + jnp.where(sends_prev, groups, 0) + jnp.where(sends_next, groups, 0)

    def wait_planes(number, options, sem):
        for option in options:
            @pl.when(number == option)
            def _(option=option):
                planes = rx.at[pl.ds(0, option)]
                pltpu.make_async_copy(planes, planes, sem).wait()

    flow_options = [groups - 1 + k * groups for k in range(3)]
    share_options = [groups - 1 + k * groups for k in range(spread)]
    wait_planes(sent_flow, flow_options, vel_send.at[0])
    wait_planes(partners, share_options, con_recv.at[0])
    for a in range(3):
        value = rx[0, a]
        for k in range(1, spread * groups):
            value = value + rx[k, a]
        out_vel[a] = value
    wait_planes(partners, share_options, con_send.at[0])


def write_kernel(advanced, velocity, out_fields, out_vel, out_sem):
    copies = [
        pltpu.make_async_copy(velocity, out_vel, out_sem.at[1]),
        pltpu.make_async_copy(advanced, out_fields, out_sem.at[0]),
    ]
    for copy in copies:
        copy.start()
    for copy in copies:
        copy.wait()


def body(subdomains, groups, velocity, pressure, fields, brownian):
    extent = velocity.shape[2]
    count, depth = fields.shape[1], fields.shape[2]
    rows = extent // LANES
    packed = rows * depth
    slots = (2 * (-(-SWEEPS // groups)) + 1) * groups

    def pack(values):
        split = values.reshape(3, count, depth, rows, LANES)
        return split.transpose(0, 1, 3, 2, 4).reshape(3, count, packed, LANES)

    dma = pltpu.SemaphoreType.DMA
    near = pl.BlockSpec(memory_space=pltpu.VMEM)
    between = pl.pallas_call(
        functools.partial(step_kernel, subdomains, groups),
        out_shape=(
            pltpu.VMEM((3, count, packed, LANES), jnp.bfloat16),
            pltpu.VMEM((3, rows, LANES), jnp.float32),
        ),
        in_specs=[pl.BlockSpec(memory_space=pltpu.HBM)] * 4,
        out_specs=(near,) * 2,
        scratch_shapes=[
            pltpu.VMEM((3, count, packed, LANES), jnp.bfloat16),
            pltpu.VMEM((3, count, packed, LANES), jnp.bfloat16),
            pltpu.VMEM((3, count, packed, LANES), jnp.float32),
            pltpu.VMEM((3, count, packed, LANES), jnp.float32),
            pltpu.VMEM((groups + 2, 3, rows, LANES), jnp.float32),
            pltpu.VMEM((rows, LANES), jnp.float32),
            pltpu.VMEM((groups, 6, rows, LANES), jnp.float32),
            pltpu.VMEM((groups, 6, rows, LANES), jnp.float32),
            pltpu.VMEM((6, rows, LANES), jnp.float32),
            pltpu.VMEM((slots, 3, rows, LANES), jnp.float32),
            pltpu.VMEM((slots, 3, rows, LANES), jnp.float32),
            dma((CHUNKS,)),
            dma((2,)),
            dma((1,)),
            dma((1,)),
            dma((2,)),
            dma((1,)),
            dma((1,)),
            pltpu.SemaphoreType.REGULAR,
        ],
        compiler_params=pltpu.CompilerParams(
            collective_id=0, has_side_effects=True, vmem_limit_bytes=VMEM_LIMIT
        ),
    )(
        *(
            pltpu.with_memory_space_constraint(values, pltpu.HBM)
            for values in (
                velocity.reshape(3, rows, LANES),
                pressure.reshape(rows, LANES),
                pack(fields),
                pack(brownian),
            )
        )
    )
    new_fields, new_velocity = pl.pallas_call(
        write_kernel,
        out_shape=(
            jax.ShapeDtypeStruct((3, count, packed, LANES), jnp.bfloat16),
            jax.ShapeDtypeStruct((3, rows, LANES), jnp.float32),
        ),
        in_specs=[near] * 2,
        out_specs=(pl.BlockSpec(memory_space=pltpu.HBM),) * 2,
        scratch_shapes=[dma((2,))],
        compiler_params=pltpu.CompilerParams(vmem_limit_bytes=VMEM_LIMIT),
    )(*between)
    unpacked = new_fields.reshape(3, count, rows, depth, LANES).transpose(0, 1, 3, 2, 4)
    return (
        unpacked.reshape(3, count, depth, extent),
        new_velocity.reshape(3, 1, extent),
    )


def solution(mesh):
    placed = (
        P(None, ("mesh", "field"), None),
        P(("mesh", "field"), None),
        P(None, "field", "mesh", None),
        P(None, "field", "mesh", None),
    )
    return jax.shard_map(
        functools.partial(body, mesh.shape["mesh"], mesh.shape["field"]),
        mesh=mesh,
        in_specs=placed,
        out_specs=(P(None, "field", "mesh", None), P(None, ("mesh", "field"), None)),
        check_vma=False,
    )
```

```python
import functools

import jax
import jax.numpy as jnp
from jax import lax
from jax.experimental import pallas as pl
from jax.experimental.pallas import tpu as pltpu
from jax.sharding import PartitionSpec as P

NY = 32
NZ = 32
SWEEPS = 4
LANES = 128
CHUNKS = 4
EARLY_CHUNKS = 0
UNROLL = 32
VMEM_LIMIT = 24 * 1024 * 1024

time_step = 0.02
axial_weight = 400.0
transverse_weight = 40.0
weissenberg = 0.5
max_stretch = 50.0
polymer_viscosity = 40.0
noise_scale = (0.02 / 0.5) ** 0.5
diagonal_weight = 1.0 / 0.02 + 2.0 * 400.0 + 4.0 * 40.0
index_table = ((0, 1, 2), (1, 3, 4), (2, 4, 5))
component_pairs = ((0, 0), (0, 1), (0, 2), (1, 1), (1, 2), (2, 2))
diagonal_pairs = (0, 3, 5)


def plane_shifts(x):
    rows = x.shape[0]
    lane = lax.broadcasted_iota(jnp.int32, x.shape, 1)
    row = lax.broadcasted_iota(jnp.int32, x.shape, 0)
    column = lane % NZ
    ahead = pltpu.roll(x, LANES - NZ, 1)
    ahead_next = jnp.where(row == rows - 1, 0.0, pltpu.roll(ahead, rows - 1, 0))
    y_plus = jnp.where(lane >= LANES - NZ, ahead_next, ahead)
    behind = pltpu.roll(x, NZ, 1)
    behind_next = jnp.where(row == 0, 0.0, pltpu.roll(behind, 1, 0))
    y_minus = jnp.where(lane < NZ, behind_next, behind)
    z_plus = jnp.where(column < NZ - 1, pltpu.roll(x, LANES - 1, 1), 0.0)
    z_minus = jnp.where(column > 0, pltpu.roll(x, 1, 1), 0.0)
    return y_plus, y_minus, z_plus, z_minus


def add(left, right):
    if left is None:
        return right
    return left if right is None else left + right


def step_kernel(
    subdomains, groups,
    vel, prs, fld, brn, advanced, out_vel,
    cur, noise, now32, next32, vbuf, pbuf, grads, stress, terms, tx, rx,
    load_sem, flow_sem, vel_send, vel_mates, vel_cross, con_send, con_recv, ready,
):
    rows = vel.shape[1]
    count = fld.shape[1]
    packed = fld.shape[2]
    total = subdomains * groups
    block = min(16, packed)
    chunk = count // CHUNKS
    reach = -(-SWEEPS // groups)
    spread = 2 * reach + 1
    sub = lax.axis_index("mesh")
    own = lax.axis_index("field")
    has_prev = sub > 0
    has_next = sub < subdomains - 1

    def inside(shift):
        return (sub + shift >= 0) & (sub + shift < subdomains)

    flow_loads = [
        pltpu.make_async_copy(vel, vbuf.at[own + 1], flow_sem.at[0]),
        pltpu.make_async_copy(prs, pbuf, flow_sem.at[1]),
    ]
    for copy in flow_loads:
        copy.start()

    barrier = pltpu.get_barrier_semaphore()

    def greet(device):
        pl.semaphore_signal(
            barrier, inc=1, device_id=device, device_id_type=pl.DeviceIdType.MESH
        )

    @pl.when(has_next)
    def _():
        greet((sub + 1, 0))

    @pl.when(has_prev)
    def _():
        greet((sub - 1, groups - 1))

    for f in range(groups):
        gathers = own != f
        if f == 0:
            gathers = gathers & jnp.logical_not(has_prev)
        if f == groups - 1:
            gathers = gathers & jnp.logical_not(has_next)

        @pl.when(gathers)
        def _(f=f):
            greet((sub, f))

    for number in range(CHUNKS):
        part = pl.ds(number * chunk, chunk)
        for copy in (
            pltpu.make_async_copy(fld.at[:, part], cur.at[:, part], load_sem.at[number]),
            pltpu.make_async_copy(brn.at[:, part], noise.at[:, part], load_sem.at[number]),
        ):
            copy.start()

    @pl.when(jnp.logical_not(has_prev))
    def _():
        vbuf[0] = jnp.zeros(vbuf.shape[1:], jnp.float32)

    @pl.when(jnp.logical_not(has_next))
    def _():
        vbuf[groups + 1] = jnp.zeros(vbuf.shape[1:], jnp.float32)

    for shift in range(-reach, reach + 1):
        if shift != 0:
            @pl.when(jnp.logical_not(inside(shift)))
            def _(shift=shift):
                rx[pl.ds((reach + shift) * groups, groups)] = jnp.zeros(
                    (groups,) + rx.shape[1:], jnp.float32
                )

    relax = time_step * max_stretch / (2.0 * weissenberg)

    def base_chunk(number):
        both = pl.ds(0, 2 * chunk)
        pltpu.make_async_copy(fld.at[:, both], cur.at[:, both], load_sem.at[number]).wait()

        @pl.loop(number * chunk, (number + 1) * chunk, unroll=2)
        def _(n):
            for start in range(0, packed, block):
                at = pl.ds(start, block)
                now = [cur[c, n, at].astype(jnp.float32) for c in range(3)]
                square = now[0] * now[0] + now[1] * now[1] + now[2] * now[2]
                keep = 1.0 - relax * (1.0 / (max_stretch - square))
                for c in range(3):
                    now32[c, n, at] = now[c]
                    next32[c, n, at] = now[c] * keep + noise_scale * noise[c, n, at].astype(jnp.float32)

    for number in range(EARLY_CHUNKS):
        base_chunk(number)

    sends_prev = (own == 0) & has_prev
    sends_next = (own == groups - 1) & has_next
    guided = sends_prev | sends_next

    @pl.when(jnp.logical_not(guided))
    def _():
        pl.semaphore_wait(barrier, groups - 1)

    def admit(helper, device, needed):
        @pl.when((own == helper) & needed)
        def _():
            pl.semaphore_signal(
                ready, inc=1, device_id=(sub, device), device_id_type=pl.DeviceIdType.MESH
            )

    admit(1, 0, has_prev)
    admit(groups - 2, groups - 1, has_next)

    for copy in flow_loads:
        copy.wait()

    @pl.when(guided)
    def _():
        pl.semaphore_wait(ready, 1)

    def flow_copy(device, slot, recv):
        return pltpu.make_async_remote_copy(
            src_ref=vbuf.at[own + 1], dst_ref=vbuf.at[slot],
            send_sem=vel_send.at[0], recv_sem=recv,
            device_id=device, device_id_type=pl.DeviceIdType.MESH,
        )

    half = max(1, groups // 2)
    across_first = (own // half + 1) * half

    def to_mates(send):
        for r in range(groups):
            f = (across_first + r) % groups

            @pl.when(f != own)
            def _(f=f):
                send(f).start()

    to_mates(lambda f: flow_copy((sub, f), own + 1, vel_mates.at[0]))

    @pl.when(sends_prev)
    def _():
        pl.semaphore_wait(barrier, groups)
        for f in sorted(range(groups), key=lambda f: (f % 2, -f)):
            flow_copy((sub - 1, f), groups + 1, vel_cross.at[1]).start()

    @pl.when(sends_next)
    def _():
        pl.semaphore_wait(barrier, groups)
        for f in sorted(range(groups), key=lambda f: (f % 2, f)):
            flow_copy((sub + 1, f), 0, vel_cross.at[0]).start()

    for number in range(EARLY_CHUNKS, CHUNKS):
        base_chunk(number)

    factor = polymer_viscosity / weissenberg

    scale = 0.5 * time_step

    def plane_fields(q):
        g = [None] * 9
        for a in range(3):
            g[3 * a] = (vbuf[q + 2, a] - vbuf[q, a]) * scale
            g[3 * a + 1] = grads[q, a]
            g[3 * a + 2] = grads[q, 3 + a]
        at = pl.ds(q, rows, stride=groups)

        def one_field(n, acc):
            now = [now32[c, n, at] for c in range(3)]
            new = []
            for a in range(3):
                value = next32[a, n, at] + (
                    g[3 * a] * now[0] + g[3 * a + 1] * now[1] + g[3 * a + 2] * now[2]
                )
                next32[a, n, at] = value
                new.append(value)
            square = new[0] * new[0] + new[1] * new[1] + new[2] * new[2]
            inverse = 1.0 / (max_stretch - square)
            pulled = [inverse * value for value in new]
            return tuple(
                total_k + pulled[left] * new[right]
                for total_k, (left, right) in zip(acc, component_pairs)
            )

        zero = jnp.zeros((rows, LANES), jnp.float32)
        acc = lax.fori_loop(0, count, one_field, (zero,) * 6, unroll=UNROLL)
        for k in range(6):
            value = acc[k] * (factor * max_stretch / (count * groups))
            stress[q, k] = value - factor / groups if k in diagonal_pairs else value

    across = (
        lax.broadcasted_iota(jnp.int32, (rows, LANES), 0) * (LANES // NZ)
        + lax.broadcasted_iota(jnp.int32, (rows, LANES), 1) // NZ
    )
    solid = jnp.where((across < NY // 4) | (across >= NY - NY // 4), 1.0, 0.0)
    first, last = -reach * groups, groups - 1 + reach * groups
    mine = [jnp.where(own == q, 1.0, 0.0) for q in range(groups)]
    y_plus, y_minus, z_plus, z_minus = plane_shifts(pbuf[...])
    pressure_slopes = (None, y_plus - y_minus, z_plus - z_minus)
    for a in range(3):
        mid = vbuf[own + 1, a]
        y_plus, y_minus, z_plus, z_minus = plane_shifts(mid)
        terms[a] = transverse_weight * ((y_plus + y_minus) + (z_plus + z_minus))
        value = mid * (1.0 / time_step)
        terms[3 + a] = value if a == 0 else value - 0.5 * pressure_slopes[a]

    def fluid(d):
        plane = sub * groups + d
        exists = jnp.where((plane >= 0) & (plane < total), 1.0 / diagonal_weight, 0.0)
        narrow = jnp.where(plane >= total // 2, 1.0, 0.0)
        return exists * (1.0 - narrow * solid)

    def momentum(outputs):
        needs = {SWEEPS: sorted(outputs)}
        for sweep in range(SWEEPS, 1, -1):
            around = {d + e for d in needs[sweep] for e in (-1, 0, 1)}
            needs[sweep - 1] = sorted(
                d for d in around if -sweep < d < groups + sweep - 1
            )
        scale_of = {}
        source = {}
        start = {}
        for d in sorted({d for ds in needs.values() for d in ds}):
            scale_of[d] = fluid(d)
            if not -1 <= d <= groups:
                continue
            along_y = {}
            along_z = {}
            if 0 <= d < groups:
                for k in range(1, 6):
                    y_plus, y_minus, z_plus, z_minus = plane_shifts(stress[d, k])
                    along_y[k] = y_plus - y_minus
                    along_z[k] = z_plus - z_minus
            for a in range(3):
                slope = None
                beside = 0.0
                for e, sign in ((1, 1.0), (-1, -1.0)):
                    if 0 <= d + e < groups:
                        other = stress[d + e, a]
                        if a == 0:
                            other = other - mine[d + e] * pbuf[...]
                        slope = add(slope, sign * other)
                        beside = beside + mine[d + e]
                if 0 <= d < groups:
                    slope = add(slope, along_y[index_table[a][1]] + along_z[index_table[a][2]])
                value = 0.5 * slope
                begin = (axial_weight * beside) * vbuf[own + 1, a]
                if 0 <= d < groups:
                    value = value + mine[d] * terms[3 + a]
                    begin = begin + mine[d] * terms[a]
                source[d, a] = scale_of[d] * value
                start[d, a] = source[d, a] + scale_of[d] * begin
        pull = {d: value * transverse_weight for d, value in scale_of.items()}
        ratio = axial_weight / transverse_weight
        v = {(d, a): start[d, a] for d in needs[1] for a in range(3)}
        for sweep in range(2, SWEEPS + 1):
            fresh = {}
            for d in needs[sweep]:
                for a in range(3):
                    value = add(v.get((d + 1, a)), v.get((d - 1, a)))
                    if value is not None:
                        value = value * ratio
                    if (d, a) in v:
                        y_plus, y_minus, z_plus, z_minus = plane_shifts(v[d, a])
                        value = add(value, (y_plus + y_minus) + (z_plus + z_minus))
                    fresh[d, a] = add(source.get((d, a)), pull[d] * value)
            v = fresh
        for d in outputs:
            for a in range(3):
                tx[d - first, a] = v[d, a]

    def share(shift, f):
        return pltpu.make_async_remote_copy(
            src_ref=tx.at[(reach + shift) * groups + f],
            dst_ref=rx.at[(reach - shift) * groups + own],
            send_sem=con_send.at[0], recv_sem=con_recv.at[0],
            device_id=(sub + shift, f), device_id_type=pl.DeviceIdType.MESH,
        )

    pltpu.make_async_copy(
        vbuf.at[pl.ds(0, groups - 1)], vbuf.at[pl.ds(0, groups - 1)], vel_mates.at[0]
    ).wait()
    for q in range(groups):
        for a in range(3):
            y_plus, y_minus, z_plus, z_minus = plane_shifts(vbuf[q + 1, a])
            grads[q, a] = (y_plus - y_minus) * scale
            grads[q, 3 + a] = (z_plus - z_minus) * scale
    for q in range(1, groups - 1):
        plane_fields(q)

    @pl.when(has_prev)
    def _():
        pltpu.make_async_copy(vbuf.at[0], vbuf.at[0], vel_cross.at[0]).wait()

    plane_fields(0)

    early = groups - 1 - SWEEPS - first

    @pl.when(has_prev)
    def _():
        momentum([first])
        share(-reach, 0).start()
        momentum(range(first + 1, first + early))
        for r in range(groups):
            f = (across_first + r) % groups

            @pl.when((f > 0) & (f < early))
            def _(f=f):
                share(-reach, f).start()

    @pl.when(has_next)
    def _():
        pltpu.make_async_copy(vbuf.at[0], vbuf.at[0], vel_cross.at[1]).wait()

    plane_fields(groups - 1)
    def share_next():
        for r in range(groups):
            share(reach, (across_first + r) % groups).start()

    @pl.when(has_prev)
    def _():
        @pl.when(has_next)
        def _():
            momentum(range(groups, last + 1))
            share_next()

        momentum(range(first + early, groups))
        for f in range(early, groups):
            share(-reach, f).start()
        to_mates(lambda f: share(0, f))

    @pl.when(jnp.logical_not(has_prev))
    def _():
        momentum(range(0, last + 1))
        to_mates(lambda f: share(0, f))
        pl.when(has_next)(share_next)

    here = reach * groups + own
    rx[here] = tx[here]

    @pl.loop(0, count, unroll=2)
    def _(n):
        for c in range(3):
            for start in range(0, packed, block):
                at = pl.ds(start, block)
                advanced[c, n, at] = next32[c, n, at].astype(jnp.bfloat16)

    partners = groups - 1
    for shift in range(-reach, reach + 1):
        if shift != 0:
            partners = partners + jnp.where(inside(shift), groups, 0)
    sent_flow = groups - 1 + jnp.where(sends_prev, groups, 0) + jnp.where(sends_next, groups, 0)

    def wait_planes(number, options, sem):
        for option in options:
            @pl.when(number == option)
            def _(option=option):
                planes = rx.at[pl.ds(0, option)]
                pltpu.make_async_copy(planes, planes, sem).wait()

    flow_options = [groups - 1 + k * groups for k in range(3)]
    share_options = [groups - 1 + k * groups for k in range(spread)]
    wait_planes(sent_flow, flow_options, vel_send.at[0])
    wait_planes(partners, share_options, con_recv.at[0])
    for a in range(3):
        value = rx[0, a]
        for k in range(1, spread * groups):
            value = value + rx[k, a]
        out_vel[a] = value
    wait_planes(partners, share_options, con_send.at[0])


def write_kernel(advanced, velocity, out_fields, out_vel, out_sem):
    copies = [
        pltpu.make_async_copy(velocity, out_vel, out_sem.at[1]),
        pltpu.make_async_copy(advanced, out_fields, out_sem.at[0]),
    ]
    for copy in copies:
        copy.start()
    for copy in copies:
        copy.wait()


def body(subdomains, groups, velocity, pressure, fields, brownian):
    extent = velocity.shape[2]
    count, depth = fields.shape[1], fields.shape[2]
    rows = extent // LANES
    packed = rows * depth
    slots = (2 * (-(-SWEEPS // groups)) + 1) * groups

    def pack(values):
        split = values.reshape(3, count, depth, rows, LANES)
        return split.transpose(0, 1, 3, 2, 4).reshape(3, count, packed, LANES)

    dma = pltpu.SemaphoreType.DMA
    near = pl.BlockSpec(memory_space=pltpu.VMEM)
    between = pl.pallas_call(
        functools.partial(step_kernel, subdomains, groups),
        out_shape=(
            pltpu.VMEM((3, count, packed, LANES), jnp.bfloat16),
            pltpu.VMEM((3, rows, LANES), jnp.float32),
        ),
        in_specs=[pl.BlockSpec(memory_space=pltpu.HBM)] * 4,
        out_specs=(near,) * 2,
        scratch_shapes=[
            pltpu.VMEM((3, count, packed, LANES), jnp.bfloat16),
            pltpu.VMEM((3, count, packed, LANES), jnp.bfloat16),
            pltpu.VMEM((3, count, packed, LANES), jnp.float32),
            pltpu.VMEM((3, count, packed, LANES), jnp.float32),
            pltpu.VMEM((groups + 2, 3, rows, LANES), jnp.float32),
            pltpu.VMEM((rows, LANES), jnp.float32),
            pltpu.VMEM((groups, 6, rows, LANES), jnp.float32),
            pltpu.VMEM((groups, 6, rows, LANES), jnp.float32),
            pltpu.VMEM((6, rows, LANES), jnp.float32),
            pltpu.VMEM((slots, 3, rows, LANES), jnp.float32),
            pltpu.VMEM((slots, 3, rows, LANES), jnp.float32),
            dma((CHUNKS,)),
            dma((2,)),
            dma((1,)),
            dma((1,)),
            dma((2,)),
            dma((1,)),
            dma((1,)),
            pltpu.SemaphoreType.REGULAR,
        ],
        compiler_params=pltpu.CompilerParams(
            collective_id=0, has_side_effects=True, vmem_limit_bytes=VMEM_LIMIT
        ),
    )(
        *(
            pltpu.with_memory_space_constraint(values, pltpu.HBM)
            for values in (
                velocity.reshape(3, rows, LANES),
                pressure.reshape(rows, LANES),
                pack(fields),
                pack(brownian),
            )
        )
    )
    new_fields, new_velocity = pl.pallas_call(
        write_kernel,
        out_shape=(
            jax.ShapeDtypeStruct((3, count, packed, LANES), jnp.bfloat16),
            jax.ShapeDtypeStruct((3, rows, LANES), jnp.float32),
        ),
        in_specs=[near] * 2,
        out_specs=(pl.BlockSpec(memory_space=pltpu.HBM),) * 2,
        scratch_shapes=[dma((2,))],
        compiler_params=pltpu.CompilerParams(vmem_limit_bytes=VMEM_LIMIT),
    )(*between)
    unpacked = new_fields.reshape(3, count, rows, depth, LANES).transpose(0, 1, 3, 2, 4)
    return (
        unpacked.reshape(3, count, depth, extent),
        new_velocity.reshape(3, 1, extent),
    )


def solution(mesh):
    placed = (
        P(None, ("mesh", "field"), None),
        P(("mesh", "field"), None),
        P(None, "field", "mesh", None),
        P(None, "field", "mesh", None),
    )
    return jax.shard_map(
        functools.partial(body, mesh.shape["mesh"], mesh.shape["field"]),
        mesh=mesh,
        in_specs=placed,
        out_specs=(P(None, "field", "mesh", None), P(None, ("mesh", "field"), None)),
        check_vma=False,
    )
```

```python
import functools

import jax
import jax.numpy as jnp
from jax import lax
from jax.experimental import pallas as pl
from jax.experimental.pallas import tpu as pltpu
from jax.sharding import PartitionSpec as P

NY = 32
NZ = 32
SWEEPS = 4
LANES = 128
CHUNKS = 2
EARLY_CHUNKS = 0
UNROLL = 32
VMEM_LIMIT = 24 * 1024 * 1024

time_step = 0.02
axial_weight = 400.0
transverse_weight = 40.0
weissenberg = 0.5
max_stretch = 50.0
polymer_viscosity = 40.0
noise_scale = (0.02 / 0.5) ** 0.5
diagonal_weight = 1.0 / 0.02 + 2.0 * 400.0 + 4.0 * 40.0
index_table = ((0, 1, 2), (1, 3, 4), (2, 4, 5))
component_pairs = ((0, 0), (0, 1), (0, 2), (1, 1), (1, 2), (2, 2))
diagonal_pairs = (0, 3, 5)


def plane_shifts(x):
    rows = x.shape[0]
    lane = lax.broadcasted_iota(jnp.int32, x.shape, 1)
    row = lax.broadcasted_iota(jnp.int32, x.shape, 0)
    column = lane % NZ
    ahead = pltpu.roll(x, LANES - NZ, 1)
    ahead_next = jnp.where(row == rows - 1, 0.0, pltpu.roll(ahead, rows - 1, 0))
    y_plus = jnp.where(lane >= LANES - NZ, ahead_next, ahead)
    behind = pltpu.roll(x, NZ, 1)
    behind_next = jnp.where(row == 0, 0.0, pltpu.roll(behind, 1, 0))
    y_minus = jnp.where(lane < NZ, behind_next, behind)
    z_plus = jnp.where(column < NZ - 1, pltpu.roll(x, LANES - 1, 1), 0.0)
    z_minus = jnp.where(column > 0, pltpu.roll(x, 1, 1), 0.0)
    return y_plus, y_minus, z_plus, z_minus


def add(left, right):
    if left is None:
        return right
    return left if right is None else left + right


def step_kernel(
    subdomains, groups,
    vel, prs, fld, brn, advanced, out_vel,
    cur, noise, now32, next32, vbuf, pbuf, grads, stress, terms, tx, rx,
    load_sem, flow_sem, send_sem, vel_mates, vel_cross, con_recv, ready,
):
    rows = vel.shape[1]
    count = fld.shape[1]
    packed = fld.shape[2]
    total = subdomains * groups
    block = min(16, packed)
    chunk = count // CHUNKS
    reach = -(-SWEEPS // groups)
    spread = 2 * reach + 1
    sub = lax.axis_index("mesh")
    own = lax.axis_index("field")
    has_prev = sub > 0
    has_next = sub < subdomains - 1

    def inside(shift):
        return (sub + shift >= 0) & (sub + shift < subdomains)

    flow_loads = [
        pltpu.make_async_copy(vel, vbuf.at[own + 1], flow_sem.at[0]),
        pltpu.make_async_copy(prs, pbuf, flow_sem.at[0]),
    ]
    for copy in flow_loads:
        copy.start()

    barrier = pltpu.get_barrier_semaphore()

    def greet(device):
        pl.semaphore_signal(
            barrier, inc=1, device_id=device, device_id_type=pl.DeviceIdType.MESH
        )

    @pl.when(has_next)
    def _():
        greet((sub + 1, 0))

    @pl.when(has_prev)
    def _():
        greet((sub - 1, groups - 1))

    for f in range(groups):
        gathers = own != f
        if f == 0:
            gathers = gathers & jnp.logical_not(has_prev)
        if f == groups - 1:
            gathers = gathers & jnp.logical_not(has_next)

        @pl.when(gathers)
        def _(f=f):
            greet((sub, f))

    for number in range(CHUNKS):
        part = pl.ds(number * chunk, chunk)
        for copy in (
            pltpu.make_async_copy(fld.at[:, part], cur.at[:, part], load_sem.at[number]),
            pltpu.make_async_copy(brn.at[:, part], noise.at[:, part], load_sem.at[number]),
        ):
            copy.start()

    @pl.when(jnp.logical_not(has_prev))
    def _():
        vbuf[0] = jnp.zeros(vbuf.shape[1:], jnp.float32)

    @pl.when(jnp.logical_not(has_next))
    def _():
        vbuf[groups + 1] = jnp.zeros(vbuf.shape[1:], jnp.float32)

    for shift in range(-reach, reach + 1):
        if shift != 0:
            @pl.when(jnp.logical_not(inside(shift)))
            def _(shift=shift):
                rx[pl.ds((reach + shift) * groups, groups)] = jnp.zeros(
                    (groups,) + rx.shape[1:], jnp.float32
                )

    relax = time_step * max_stretch / (2.0 * weissenberg)

    def base_chunk(number):
        both = now32.at[:, pl.ds(0, chunk)]
        pltpu.make_async_copy(both, both, load_sem.at[number]).wait()

        @pl.loop(number * chunk, (number + 1) * chunk, unroll=2)
        def _(n):
            for start in range(0, packed, block):
                at = pl.ds(start, block)
                now = [cur[c, n, at].astype(jnp.float32) for c in range(3)]
                square = now[0] * now[0] + now[1] * now[1] + now[2] * now[2]
                keep = 1.0 - relax * (1.0 / (max_stretch - square))
                for c in range(3):
                    now32[c, n, at] = now[c]
                    next32[c, n, at] = now[c] * keep + noise_scale * noise[c, n, at].astype(jnp.float32)

    for number in range(EARLY_CHUNKS):
        base_chunk(number)

    sends_prev = (own == 0) & has_prev
    sends_next = (own == groups - 1) & has_next
    guided = sends_prev | sends_next

    @pl.when(jnp.logical_not(guided))
    def _():
        pl.semaphore_wait(barrier, groups - 1)

    def admit(helper, device, needed):
        @pl.when((own == helper) & needed)
        def _():
            pl.semaphore_signal(
                ready, inc=1, device_id=(sub, device), device_id_type=pl.DeviceIdType.MESH
            )

    admit(1, 0, has_prev)
    admit(groups - 2, groups - 1, has_next)

    loaded = stress.at[0, pl.ds(0, 4)]
    pltpu.make_async_copy(loaded, loaded, flow_sem.at[0]).wait()

    @pl.when(guided)
    def _():
        pl.semaphore_wait(ready, 1)

    def flow_copy(device, slot, recv):
        return pltpu.make_async_remote_copy(
            src_ref=vbuf.at[own + 1], dst_ref=vbuf.at[slot],
            send_sem=send_sem.at[0], recv_sem=recv,
            device_id=device, device_id_type=pl.DeviceIdType.MESH,
        )

    half = max(1, groups // 2)
    across_first = (own // half + 1) * half

    def to_mates(send):
        for r in range(groups):
            f = (across_first + r) % groups

            @pl.when(f != own)
            def _(f=f):
                send(f).start()

    arrives = vel_mates.at[jnp.where(own == 0, 1, 0)]
    to_mates(lambda f: flow_copy((sub, f), own + 1, arrives))

    @pl.when(sends_prev)
    def _():
        pl.semaphore_wait(barrier, groups)
        for f in sorted(range(groups), key=lambda f: (f % 2, -f)):
            flow_copy((sub - 1, f), groups + 1, vel_cross.at[1]).start()

    @pl.when(sends_next)
    def _():
        pl.semaphore_wait(barrier, groups)
        for f in sorted(range(groups), key=lambda f: (f % 2, f)):
            flow_copy((sub + 1, f), 0, vel_cross.at[0]).start()

    for number in range(EARLY_CHUNKS, CHUNKS):
        base_chunk(number)

    factor = polymer_viscosity / weissenberg

    scale = 0.5 * time_step

    def plane_fields(q):
        g = [None] * 9
        for a in range(3):
            g[3 * a] = (vbuf[q + 2, a] - vbuf[q, a]) * scale
            g[3 * a + 1] = grads[q, a]
            g[3 * a + 2] = grads[q, 3 + a]
        at = pl.ds(q, rows, stride=groups)

        def one_field(n, acc):
            now = [now32[c, n, at] for c in range(3)]
            new = []
            for a in range(3):
                value = next32[a, n, at] + (
                    g[3 * a] * now[0] + g[3 * a + 1] * now[1] + g[3 * a + 2] * now[2]
                )
                next32[a, n, at] = value
                new.append(value)
            square = new[0] * new[0] + new[1] * new[1] + new[2] * new[2]
            inverse = 1.0 / (max_stretch - square)
            pulled = [inverse * value for value in new]
            return tuple(
                total_k + pulled[left] * new[right]
                for total_k, (left, right) in zip(acc, component_pairs)
            )

        zero = jnp.zeros((rows, LANES), jnp.float32)
        acc = lax.fori_loop(0, count, one_field, (zero,) * 6, unroll=UNROLL)
        for k in range(6):
            value = acc[k] * (factor * max_stretch / (count * groups))
            stress[q, k] = value - factor / groups if k in diagonal_pairs else value

    across = (
        lax.broadcasted_iota(jnp.int32, (rows, LANES), 0) * (LANES // NZ)
        + lax.broadcasted_iota(jnp.int32, (rows, LANES), 1) // NZ
    )
    solid = jnp.where((across < NY // 4) | (across >= NY - NY // 4), 1.0, 0.0)
    first, last = -reach * groups, groups - 1 + reach * groups
    mine = [jnp.where(own == q, 1.0, 0.0) for q in range(groups)]
    y_plus, y_minus, z_plus, z_minus = plane_shifts(pbuf[...])
    pressure_slopes = (None, y_plus - y_minus, z_plus - z_minus)
    for a in range(3):
        mid = vbuf[own + 1, a]
        y_plus, y_minus, z_plus, z_minus = plane_shifts(mid)
        terms[a] = transverse_weight * ((y_plus + y_minus) + (z_plus + z_minus))
        value = mid * (1.0 / time_step)
        terms[3 + a] = value if a == 0 else value - 0.5 * pressure_slopes[a]

    def fluid(d):
        plane = sub * groups + d
        exists = jnp.where((plane >= 0) & (plane < total), 1.0 / diagonal_weight, 0.0)
        narrow = jnp.where(plane >= total // 2, 1.0, 0.0)
        return exists * (1.0 - narrow * solid)

    def momentum(outputs):
        needs = {SWEEPS: sorted(outputs)}
        for sweep in range(SWEEPS, 1, -1):
            around = {d + e for d in needs[sweep] for e in (-1, 0, 1)}
            needs[sweep - 1] = sorted(
                d for d in around if -sweep < d < groups + sweep - 1
            )
        scale_of = {}
        source = {}
        start = {}
        for d in sorted({d for ds in needs.values() for d in ds}):
            scale_of[d] = fluid(d)
            if not -1 <= d <= groups:
                continue
            along_y = {}
            along_z = {}
            if 0 <= d < groups:
                for k in range(1, 6):
                    y_plus, y_minus, z_plus, z_minus = plane_shifts(stress[d, k])
                    along_y[k] = y_plus - y_minus
                    along_z[k] = z_plus - z_minus
            for a in range(3):
                slope = None
                beside = 0.0
                for e, sign in ((1, 1.0), (-1, -1.0)):
                    if 0 <= d + e < groups:
                        other = stress[d + e, a]
                        if a == 0:
                            other = other - mine[d + e] * pbuf[...]
                        slope = add(slope, sign * other)
                        beside = beside + mine[d + e]
                if 0 <= d < groups:
                    slope = add(slope, along_y[index_table[a][1]] + along_z[index_table[a][2]])
                value = 0.5 * slope
                begin = (axial_weight * beside) * vbuf[own + 1, a]
                if 0 <= d < groups:
                    value = value + mine[d] * terms[3 + a]
                    begin = begin + mine[d] * terms[a]
                source[d, a] = scale_of[d] * value
                start[d, a] = source[d, a] + scale_of[d] * begin
        pull = {d: value * transverse_weight for d, value in scale_of.items()}
        ratio = axial_weight / transverse_weight
        v = {(d, a): start[d, a] for d in needs[1] for a in range(3)}
        for sweep in range(2, SWEEPS + 1):
            fresh = {}
            for d in needs[sweep]:
                for a in range(3):
                    value = add(v.get((d + 1, a)), v.get((d - 1, a)))
                    if value is not None:
                        value = value * ratio
                    if (d, a) in v:
                        y_plus, y_minus, z_plus, z_minus = plane_shifts(v[d, a])
                        value = add(value, (y_plus + y_minus) + (z_plus + z_minus))
                    fresh[d, a] = add(source.get((d, a)), pull[d] * value)
            v = fresh
        for d in outputs:
            for a in range(3):
                tx[d - first, a] = v[d, a]

    def share(shift, f):
        return pltpu.make_async_remote_copy(
            src_ref=tx.at[(reach + shift) * groups + f],
            dst_ref=rx.at[(reach - shift) * groups + own],
            send_sem=send_sem.at[0], recv_sem=con_recv.at[0],
            device_id=(sub + shift, f), device_id_type=pl.DeviceIdType.MESH,
        )

    def wait_velocity(number, sem):
        planes = vbuf.at[pl.ds(0, number)]
        pltpu.make_async_copy(planes, planes, sem).wait()

    def cross_slopes(planes):
        for q in planes:
            for a in range(3):
                y_plus, y_minus, z_plus, z_minus = plane_shifts(vbuf[q + 1, a])
                grads[q, a] = (y_plus - y_minus) * scale
                grads[q, 3 + a] = (z_plus - z_minus) * scale

    @pl.when(own == 0)
    def _():
        wait_velocity(groups - 1, vel_mates.at[0])

    @pl.when(own != 0)
    def _():
        wait_velocity(groups - 2, vel_mates.at[0])

    @pl.when((own != 0) & (own < half))
    def _():
        wait_velocity(1, vel_mates.at[1])

    @pl.when(own < half)
    def _():
        cross_slopes(range(groups))

    @pl.when(own >= half)
    def _():
        cross_slopes(range(1, groups))

    for q in reversed(range(2, groups - 1)):
        plane_fields(q)

    @pl.when(own >= half)
    def _():
        wait_velocity(1, vel_mates.at[1])
        cross_slopes(range(1))

    plane_fields(1)

    @pl.when(has_prev)
    def _():
        pltpu.make_async_copy(vbuf.at[0], vbuf.at[0], vel_cross.at[0]).wait()

    plane_fields(0)

    early = groups - 1 - SWEEPS - first

    @pl.when(has_prev)
    def _():
        momentum([first])
        share(-reach, 0).start()
        momentum(range(first + 1, first + early))
        for r in range(groups):
            f = (across_first + r) % groups

            @pl.when((f > 0) & (f < early))
            def _(f=f):
                share(-reach, f).start()

    @pl.when(has_next)
    def _():
        pltpu.make_async_copy(vbuf.at[0], vbuf.at[0], vel_cross.at[1]).wait()

    plane_fields(groups - 1)
    def share_next():
        for r in range(groups):
            share(reach, (across_first + r) % groups).start()

    @pl.when(has_prev)
    def _():
        @pl.when(has_next)
        def _():
            momentum(range(groups, last + 1))
            share_next()

        momentum(range(first + early, groups))
        for f in range(early, groups):
            share(-reach, f).start()
        to_mates(lambda f: share(0, f))

    @pl.when(jnp.logical_not(has_prev))
    def _():
        momentum(range(0, groups))
        to_mates(lambda f: share(0, f))

        @pl.when(has_next)
        def _():
            momentum(range(groups, last + 1))
            share_next()

    here = reach * groups + own
    rx[here] = tx[here]

    @pl.loop(0, count, unroll=2)
    def _(n):
        for c in range(3):
            for start in range(0, packed, block):
                at = pl.ds(start, block)
                advanced[c, n, at] = next32[c, n, at].astype(jnp.bfloat16)

    partners = groups - 1
    for shift in range(-reach, reach + 1):
        if shift != 0:
            partners = partners + jnp.where(inside(shift), groups, 0)
    sent_flow = groups - 1 + jnp.where(sends_prev, groups, 0) + jnp.where(sends_next, groups, 0)

    def wait_planes(number, options, sem):
        for option in options:
            @pl.when(number == option)
            def _(option=option):
                planes = now32.at[:, pl.ds(0, option), pl.ds(0, rows)]
                pltpu.make_async_copy(planes, planes, sem).wait()

    wait_planes(partners, [groups - 1 + k * groups for k in range(spread)], con_recv.at[0])
    for a in range(3):
        value = rx[0, a]
        for k in range(1, spread * groups):
            value = value + rx[k, a]
        out_vel[a] = value
    wait_planes(
        partners + sent_flow,
        [2 * (groups - 1) + k * groups for k in range(spread + 1)],
        send_sem.at[0],
    )


def write_kernel(advanced, velocity, out_fields, out_vel, out_sem):
    copies = [
        pltpu.make_async_copy(velocity, out_vel, out_sem.at[1]),
        pltpu.make_async_copy(advanced, out_fields, out_sem.at[0]),
    ]
    for copy in copies:
        copy.start()
    for copy in copies:
        copy.wait()


def body(subdomains, groups, velocity, pressure, fields, brownian):
    extent = velocity.shape[2]
    count, depth = fields.shape[1], fields.shape[2]
    rows = extent // LANES
    packed = rows * depth
    slots = (2 * (-(-SWEEPS // groups)) + 1) * groups

    def pack(values):
        split = values.reshape(3, count, depth, rows, LANES)
        return split.transpose(0, 1, 3, 2, 4).reshape(3, count, packed, LANES)

    dma = pltpu.SemaphoreType.DMA
    near = pl.BlockSpec(memory_space=pltpu.VMEM)
    between = pl.pallas_call(
        functools.partial(step_kernel, subdomains, groups),
        out_shape=(
            pltpu.VMEM((3, count, packed, LANES), jnp.bfloat16),
            pltpu.VMEM((3, rows, LANES), jnp.float32),
        ),
        in_specs=[pl.BlockSpec(memory_space=pltpu.HBM)] * 4,
        out_specs=(near,) * 2,
        scratch_shapes=[
            pltpu.VMEM((3, count, packed, LANES), jnp.bfloat16),
            pltpu.VMEM((3, count, packed, LANES), jnp.bfloat16),
            pltpu.VMEM((3, count, packed, LANES), jnp.float32),
            pltpu.VMEM((3, count, packed, LANES), jnp.float32),
            pltpu.VMEM((groups + 2, 3, rows, LANES), jnp.float32),
            pltpu.VMEM((rows, LANES), jnp.float32),
            pltpu.VMEM((groups, 6, rows, LANES), jnp.float32),
            pltpu.VMEM((groups, 6, rows, LANES), jnp.float32),
            pltpu.VMEM((6, rows, LANES), jnp.float32),
            pltpu.VMEM((slots, 3, rows, LANES), jnp.float32),
            pltpu.VMEM((slots, 3, rows, LANES), jnp.float32),
            dma((CHUNKS,)),
            dma((1,)),
            dma((1,)),
            dma((2,)),
            dma((2,)),
            dma((1,)),
            pltpu.SemaphoreType.REGULAR,
        ],
        compiler_params=pltpu.CompilerParams(
            collective_id=0, has_side_effects=True, vmem_limit_bytes=VMEM_LIMIT
        ),
    )(
        *(
            pltpu.with_memory_space_constraint(values, pltpu.HBM)
            for values in (
                velocity.reshape(3, rows, LANES),
                pressure.reshape(rows, LANES),
                pack(fields),
                pack(brownian),
            )
        )
    )
    new_fields, new_velocity = pl.pallas_call(
        write_kernel,
        out_shape=(
            jax.ShapeDtypeStruct((3, count, packed, LANES), jnp.bfloat16),
            jax.ShapeDtypeStruct((3, rows, LANES), jnp.float32),
        ),
        in_specs=[near] * 2,
        out_specs=(pl.BlockSpec(memory_space=pltpu.HBM),) * 2,
        scratch_shapes=[dma((2,))],
        compiler_params=pltpu.CompilerParams(vmem_limit_bytes=VMEM_LIMIT),
    )(*between)
    unpacked = new_fields.reshape(3, count, rows, depth, LANES).transpose(0, 1, 3, 2, 4)
    return (
        unpacked.reshape(3, count, depth, extent),
        new_velocity.reshape(3, 1, extent),
    )


def solution(mesh):
    placed = (
        P(None, ("mesh", "field"), None),
        P(("mesh", "field"), None),
        P(None, "field", "mesh", None),
        P(None, "field", "mesh", None),
    )
    return jax.shard_map(
        functools.partial(body, mesh.shape["mesh"], mesh.shape["field"]),
        mesh=mesh,
        in_specs=placed,
        out_specs=(P(None, "field", "mesh", None), P(None, ("mesh", "field"), None)),
        check_vma=False,
    )
```

```python
import functools

import jax
import jax.numpy as jnp
from jax import lax
from jax.experimental import pallas as pl
from jax.experimental.pallas import tpu as pltpu
from jax.sharding import PartitionSpec as P

NY = 32
NZ = 32
SWEEPS = 4
LANES = 128
CHUNKS = 2
EARLY_CHUNKS = 0
UNROLL = 32
VMEM_LIMIT = 24 * 1024 * 1024

time_step = 0.02
axial_weight = 400.0
transverse_weight = 40.0
weissenberg = 0.5
max_stretch = 50.0
polymer_viscosity = 40.0
noise_scale = (0.02 / 0.5) ** 0.5
diagonal_weight = 1.0 / 0.02 + 2.0 * 400.0 + 4.0 * 40.0
index_table = ((0, 1, 2), (1, 3, 4), (2, 4, 5))
component_pairs = ((0, 0), (0, 1), (0, 2), (1, 1), (1, 2), (2, 2))
diagonal_pairs = (0, 3, 5)


def plane_shifts(x):
    rows = x.shape[0]
    lane = lax.broadcasted_iota(jnp.int32, x.shape, 1)
    row = lax.broadcasted_iota(jnp.int32, x.shape, 0)
    column = lane % NZ
    ahead = pltpu.roll(x, LANES - NZ, 1)
    ahead_next = jnp.where(row == rows - 1, 0.0, pltpu.roll(ahead, rows - 1, 0))
    y_plus = jnp.where(lane >= LANES - NZ, ahead_next, ahead)
    behind = pltpu.roll(x, NZ, 1)
    behind_next = jnp.where(row == 0, 0.0, pltpu.roll(behind, 1, 0))
    y_minus = jnp.where(lane < NZ, behind_next, behind)
    z_plus = jnp.where(column < NZ - 1, pltpu.roll(x, LANES - 1, 1), 0.0)
    z_minus = jnp.where(column > 0, pltpu.roll(x, 1, 1), 0.0)
    return y_plus, y_minus, z_plus, z_minus


def add(left, right):
    if left is None:
        return right
    return left if right is None else left + right


def step_kernel(
    subdomains, groups,
    vel, prs, fld, brn, advanced, out_vel,
    cur, noise, now32, next32, vbuf, pbuf, grads, stress, terms, tx, rx,
    load_sem, flow_sem, send_sem, vel_mates, vel_cross, con_recv, ready,
):
    rows = vel.shape[1]
    count = fld.shape[1]
    packed = fld.shape[2]
    total = subdomains * groups
    block = min(16, packed)
    chunk = count // CHUNKS
    reach = -(-SWEEPS // groups)
    spread = 2 * reach + 1
    sub = lax.axis_index("mesh")
    own = lax.axis_index("field")
    has_prev = sub > 0
    has_next = sub < subdomains - 1

    def inside(shift):
        return (sub + shift >= 0) & (sub + shift < subdomains)

    flow_loads = [
        pltpu.make_async_copy(vel, vbuf.at[own + 1], flow_sem.at[0]),
        pltpu.make_async_copy(prs, pbuf, flow_sem.at[0]),
    ]
    for copy in flow_loads:
        copy.start()

    barrier = pltpu.get_barrier_semaphore()

    def greet(device):
        pl.semaphore_signal(
            barrier, inc=1, device_id=device, device_id_type=pl.DeviceIdType.MESH
        )

    @pl.when(has_next)
    def _():
        greet((sub + 1, 0))

    @pl.when(has_prev)
    def _():
        greet((sub - 1, groups - 1))

    for f in range(groups):
        gathers = own != f
        if f == 0:
            gathers = gathers & jnp.logical_not(has_prev)
        if f == groups - 1:
            gathers = gathers & jnp.logical_not(has_next)

        @pl.when(gathers)
        def _(f=f):
            greet((sub, f))

    for number in range(CHUNKS):
        part = pl.ds(number * chunk, chunk)
        for copy in (
            pltpu.make_async_copy(fld.at[:, part], cur.at[:, part], load_sem.at[number]),
            pltpu.make_async_copy(brn.at[:, part], noise.at[:, part], load_sem.at[number]),
        ):
            copy.start()

    @pl.when(jnp.logical_not(has_prev))
    def _():
        vbuf[0] = jnp.zeros(vbuf.shape[1:], jnp.float32)

    @pl.when(jnp.logical_not(has_next))
    def _():
        vbuf[groups + 1] = jnp.zeros(vbuf.shape[1:], jnp.float32)

    for shift in range(-reach, reach + 1):
        if shift != 0:
            @pl.when(jnp.logical_not(inside(shift)))
            def _(shift=shift):
                rx[pl.ds((reach + shift) * groups, groups)] = jnp.zeros(
                    (groups,) + rx.shape[1:], jnp.float32
                )

    relax = time_step * max_stretch / (2.0 * weissenberg)

    def base_chunk(number):
        both = now32.at[:, pl.ds(0, chunk)]
        pltpu.make_async_copy(both, both, load_sem.at[number]).wait()

        @pl.loop(number * chunk, (number + 1) * chunk, unroll=2)
        def _(n):
            for start in range(0, packed, block):
                at = pl.ds(start, block)
                now = [cur[c, n, at].astype(jnp.float32) for c in range(3)]
                square = now[0] * now[0] + now[1] * now[1] + now[2] * now[2]
                keep = 1.0 - relax * (1.0 / (max_stretch - square))
                for c in range(3):
                    now32[c, n, at] = now[c]
                    next32[c, n, at] = now[c] * keep + noise_scale * noise[c, n, at].astype(jnp.float32)

    for number in range(EARLY_CHUNKS):
        base_chunk(number)

    sends_prev = (own == 0) & has_prev
    sends_next = (own == groups - 1) & has_next
    guided = sends_prev | sends_next

    @pl.when(jnp.logical_not(guided))
    def _():
        pl.semaphore_wait(barrier, groups - 1)

    def admit(helper, device, needed):
        @pl.when((own == helper) & needed)
        def _():
            pl.semaphore_signal(
                ready, inc=1, device_id=(sub, device), device_id_type=pl.DeviceIdType.MESH
            )

    admit(1, 0, has_prev)
    admit(groups - 2, groups - 1, has_next)

    loaded = stress.at[0, pl.ds(0, 4)]
    pltpu.make_async_copy(loaded, loaded, flow_sem.at[0]).wait()

    @pl.when(guided)
    def _():
        pl.semaphore_wait(ready, 1)

    def flow_copy(device, slot, recv):
        return pltpu.make_async_remote_copy(
            src_ref=vbuf.at[own + 1], dst_ref=vbuf.at[slot],
            send_sem=send_sem.at[0], recv_sem=recv,
            device_id=device, device_id_type=pl.DeviceIdType.MESH,
        )

    half = max(1, groups // 2)
    across_first = (own // half + 1) * half

    def to_mates(send):
        for r in range(groups):
            f = (across_first + r) % groups

            @pl.when(f != own)
            def _(f=f):
                send(f).start()

    arrives = vel_mates.at[jnp.where(own == 0, 1, 0)]
    to_mates(lambda f: flow_copy((sub, f), own + 1, arrives))

    @pl.when(sends_prev)
    def _():
        pl.semaphore_wait(barrier, groups)
        for f in sorted(range(groups), key=lambda f: (f % 2, -f)):
            flow_copy((sub - 1, f), groups + 1, vel_cross.at[1]).start()

    @pl.when(sends_next)
    def _():
        pl.semaphore_wait(barrier, groups)
        for f in sorted(range(groups), key=lambda f: (f % 2, f)):
            flow_copy((sub + 1, f), 0, vel_cross.at[0]).start()

    for number in range(EARLY_CHUNKS, CHUNKS):
        base_chunk(number)

    factor = polymer_viscosity / weissenberg

    scale = 0.5 * time_step

    def prepare_fields(q):
        g = [None] * 9
        for a in range(3):
            g[3 * a] = vbuf[q, a] * -scale
            g[3 * a + 1] = grads[q, a]
            g[3 * a + 2] = grads[q, 3 + a]
        at = pl.ds(q, rows, stride=groups)

        @pl.loop(0, count, unroll=UNROLL // 2)
        def _(n):
            now = [now32[c, n, at] for c in range(3)]
            for a in range(3):
                next32[a, n, at] = next32[a, n, at] + (
                    g[3 * a] * now[0] + g[3 * a + 1] * now[1] + g[3 * a + 2] * now[2]
                )

    def plane_fields(q, prepared=False):
        g = [None] * 9
        for a in range(3):
            if prepared:
                g[3 * a] = vbuf[q + 2, a] * scale
                continue
            g[3 * a] = (vbuf[q + 2, a] - vbuf[q, a]) * scale
            g[3 * a + 1] = grads[q, a]
            g[3 * a + 2] = grads[q, 3 + a]
        at = pl.ds(q, rows, stride=groups)

        def one_field(n, acc):
            now = [now32[c, n, at] for c in range(1 if prepared else 3)]
            new = []
            for a in range(3):
                stretch = g[3 * a] * now[0]
                if not prepared:
                    stretch = stretch + g[3 * a + 1] * now[1] + g[3 * a + 2] * now[2]
                value = next32[a, n, at] + stretch
                next32[a, n, at] = value
                new.append(value)
            square = new[0] * new[0] + new[1] * new[1] + new[2] * new[2]
            inverse = 1.0 / (max_stretch - square)
            pulled = [inverse * value for value in new]
            return tuple(
                total_k + pulled[left] * new[right]
                for total_k, (left, right) in zip(acc, component_pairs)
            )

        zero = jnp.zeros((rows, LANES), jnp.float32)
        acc = lax.fori_loop(0, count, one_field, (zero,) * 6, unroll=UNROLL)
        for k in range(6):
            value = acc[k] * (factor * max_stretch / (count * groups))
            stress[q, k] = value - factor / groups if k in diagonal_pairs else value

    across = (
        lax.broadcasted_iota(jnp.int32, (rows, LANES), 0) * (LANES // NZ)
        + lax.broadcasted_iota(jnp.int32, (rows, LANES), 1) // NZ
    )
    solid = jnp.where((across < NY // 4) | (across >= NY - NY // 4), 1.0, 0.0)
    first, last = -reach * groups, groups - 1 + reach * groups
    mine = [jnp.where(own == q, 1.0, 0.0) for q in range(groups)]
    y_plus, y_minus, z_plus, z_minus = plane_shifts(pbuf[...])
    pressure_slopes = (None, y_plus - y_minus, z_plus - z_minus)
    for a in range(3):
        mid = vbuf[own + 1, a]
        y_plus, y_minus, z_plus, z_minus = plane_shifts(mid)
        terms[a] = transverse_weight * ((y_plus + y_minus) + (z_plus + z_minus))
        value = mid * (1.0 / time_step)
        terms[3 + a] = value if a == 0 else value - 0.5 * pressure_slopes[a]

    def fluid(d):
        plane = sub * groups + d
        exists = jnp.where((plane >= 0) & (plane < total), 1.0 / diagonal_weight, 0.0)
        narrow = jnp.where(plane >= total // 2, 1.0, 0.0)
        return exists * (1.0 - narrow * solid)

    def momentum(outputs):
        needs = {SWEEPS: sorted(outputs)}
        for sweep in range(SWEEPS, 1, -1):
            around = {d + e for d in needs[sweep] for e in (-1, 0, 1)}
            needs[sweep - 1] = sorted(
                d for d in around if -sweep < d < groups + sweep - 1
            )
        scale_of = {}
        source = {}
        start = {}
        for d in sorted({d for ds in needs.values() for d in ds}):
            scale_of[d] = fluid(d)
            if not -1 <= d <= groups:
                continue
            along_y = {}
            along_z = {}
            if 0 <= d < groups:
                for k in range(1, 6):
                    y_plus, y_minus, z_plus, z_minus = plane_shifts(stress[d, k])
                    along_y[k] = y_plus - y_minus
                    along_z[k] = z_plus - z_minus
            for a in range(3):
                slope = None
                beside = 0.0
                for e, sign in ((1, 1.0), (-1, -1.0)):
                    if 0 <= d + e < groups:
                        other = stress[d + e, a]
                        if a == 0:
                            other = other - mine[d + e] * pbuf[...]
                        slope = add(slope, sign * other)
                        beside = beside + mine[d + e]
                if 0 <= d < groups:
                    slope = add(slope, along_y[index_table[a][1]] + along_z[index_table[a][2]])
                value = 0.5 * slope
                begin = (axial_weight * beside) * vbuf[own + 1, a]
                if 0 <= d < groups:
                    value = value + mine[d] * terms[3 + a]
                    begin = begin + mine[d] * terms[a]
                source[d, a] = scale_of[d] * value
                start[d, a] = source[d, a] + scale_of[d] * begin
        pull = {d: value * transverse_weight for d, value in scale_of.items()}
        ratio = axial_weight / transverse_weight
        v = {(d, a): start[d, a] for d in needs[1] for a in range(3)}
        for sweep in range(2, SWEEPS + 1):
            fresh = {}
            for d in needs[sweep]:
                for a in range(3):
                    value = add(v.get((d + 1, a)), v.get((d - 1, a)))
                    if value is not None:
                        value = value * ratio
                    if (d, a) in v:
                        y_plus, y_minus, z_plus, z_minus = plane_shifts(v[d, a])
                        value = add(value, (y_plus + y_minus) + (z_plus + z_minus))
                    fresh[d, a] = add(source.get((d, a)), pull[d] * value)
            v = fresh
        for d in outputs:
            for a in range(3):
                tx[d - first, a] = v[d, a]

    def share(shift, f):
        return pltpu.make_async_remote_copy(
            src_ref=tx.at[(reach + shift) * groups + f],
            dst_ref=rx.at[(reach - shift) * groups + own],
            send_sem=send_sem.at[0], recv_sem=con_recv.at[0],
            device_id=(sub + shift, f), device_id_type=pl.DeviceIdType.MESH,
        )

    def wait_velocity(number, sem):
        planes = vbuf.at[pl.ds(0, number)]
        pltpu.make_async_copy(planes, planes, sem).wait()

    def cross_slopes(planes):
        for q in planes:
            for a in range(3):
                y_plus, y_minus, z_plus, z_minus = plane_shifts(vbuf[q + 1, a])
                grads[q, a] = (y_plus - y_minus) * scale
                grads[q, 3 + a] = (z_plus - z_minus) * scale

    @pl.when(own == 0)
    def _():
        wait_velocity(groups - 1, vel_mates.at[0])

    @pl.when(own != 0)
    def _():
        wait_velocity(groups - 2, vel_mates.at[0])

    @pl.when((own != 0) & (own < half))
    def _():
        wait_velocity(1, vel_mates.at[1])

    @pl.when(own < half)
    def _():
        cross_slopes(range(groups))

    @pl.when(own >= half)
    def _():
        cross_slopes(range(1, groups))

    for q in reversed(range(2, groups - 1)):
        plane_fields(q)

    @pl.when(own >= half)
    def _():
        wait_velocity(1, vel_mates.at[1])
        cross_slopes(range(1))

    plane_fields(1)

    @pl.when(has_prev)
    def _():
        pltpu.make_async_copy(vbuf.at[0], vbuf.at[0], vel_cross.at[0]).wait()

    plane_fields(0)

    early = groups - 1 - SWEEPS - first

    @pl.when(has_prev)
    def _():
        momentum([first])
        share(-reach, 0).start()
        momentum(range(first + 1, first + early))
        for r in range(groups):
            f = (across_first + r) % groups

            @pl.when((f > 0) & (f < early))
            def _(f=f):
                share(-reach, f).start()

    prepare_fields(groups - 1)

    @pl.when(has_next)
    def _():
        pltpu.make_async_copy(vbuf.at[0], vbuf.at[0], vel_cross.at[1]).wait()

    plane_fields(groups - 1, True)
    def share_next():
        for r in range(groups):
            share(reach, (across_first + r) % groups).start()

    @pl.when(has_prev)
    def _():
        @pl.when(has_next)
        def _():
            momentum(range(groups, last + 1))
            share_next()

        momentum(range(first + early, groups))
        for f in range(early, groups):
            share(-reach, f).start()
        to_mates(lambda f: share(0, f))

    @pl.when(jnp.logical_not(has_prev))
    def _():
        momentum(range(0, groups))
        to_mates(lambda f: share(0, f))

        @pl.when(has_next)
        def _():
            momentum(range(groups, last + 1))
            share_next()

    here = reach * groups + own
    rx[here] = tx[here]

    @pl.loop(0, count, unroll=2)
    def _(n):
        for c in range(3):
            for start in range(0, packed, block):
                at = pl.ds(start, block)
                advanced[c, n, at] = next32[c, n, at].astype(jnp.bfloat16)

    partners = groups - 1
    for shift in range(-reach, reach + 1):
        if shift != 0:
            partners = partners + jnp.where(inside(shift), groups, 0)
    sent_flow = groups - 1 + jnp.where(sends_prev, groups, 0) + jnp.where(sends_next, groups, 0)

    def wait_planes(number, options, sem):
        for option in options:
            @pl.when(number == option)
            def _(option=option):
                planes = now32.at[:, pl.ds(0, option), pl.ds(0, rows)]
                pltpu.make_async_copy(planes, planes, sem).wait()

    wait_planes(partners, [groups - 1 + k * groups for k in range(spread)], con_recv.at[0])
    for a in range(3):
        value = rx[0, a]
        for k in range(1, spread * groups):
            value = value + rx[k, a]
        out_vel[a] = value
    wait_planes(
        partners + sent_flow,
        [2 * (groups - 1) + k * groups for k in range(spread + 1)],
        send_sem.at[0],
    )


def write_kernel(advanced, velocity, out_fields, out_vel, out_sem):
    copies = [
        pltpu.make_async_copy(velocity, out_vel, out_sem.at[1]),
        pltpu.make_async_copy(advanced, out_fields, out_sem.at[0]),
    ]
    for copy in copies:
        copy.start()
    for copy in copies:
        copy.wait()


def body(subdomains, groups, velocity, pressure, fields, brownian):
    extent = velocity.shape[2]
    count, depth = fields.shape[1], fields.shape[2]
    rows = extent // LANES
    packed = rows * depth
    slots = (2 * (-(-SWEEPS // groups)) + 1) * groups

    def pack(values):
        split = values.reshape(3, count, depth, rows, LANES)
        return split.transpose(0, 1, 3, 2, 4).reshape(3, count, packed, LANES)

    dma = pltpu.SemaphoreType.DMA
    near = pl.BlockSpec(memory_space=pltpu.VMEM)
    between = pl.pallas_call(
        functools.partial(step_kernel, subdomains, groups),
        out_shape=(
            pltpu.VMEM((3, count, packed, LANES), jnp.bfloat16),
            pltpu.VMEM((3, rows, LANES), jnp.float32),
        ),
        in_specs=[pl.BlockSpec(memory_space=pltpu.HBM)] * 4,
        out_specs=(near,) * 2,
        scratch_shapes=[
            pltpu.VMEM((3, count, packed, LANES), jnp.bfloat16),
            pltpu.VMEM((3, count, packed, LANES), jnp.bfloat16),
            pltpu.VMEM((3, count, packed, LANES), jnp.float32),
            pltpu.VMEM((3, count, packed, LANES), jnp.float32),
            pltpu.VMEM((groups + 2, 3, rows, LANES), jnp.float32),
            pltpu.VMEM((rows, LANES), jnp.float32),
            pltpu.VMEM((groups, 6, rows, LANES), jnp.float32),
            pltpu.VMEM((groups, 6, rows, LANES), jnp.float32),
            pltpu.VMEM((6, rows, LANES), jnp.float32),
            pltpu.VMEM((slots, 3, rows, LANES), jnp.float32),
            pltpu.VMEM((slots, 3, rows, LANES), jnp.float32),
            dma((CHUNKS,)),
            dma((1,)),
            dma((1,)),
            dma((2,)),
            dma((2,)),
            dma((1,)),
            pltpu.SemaphoreType.REGULAR,
        ],
        compiler_params=pltpu.CompilerParams(
            collective_id=0, has_side_effects=True, vmem_limit_bytes=VMEM_LIMIT
        ),
    )(
        *(
            pltpu.with_memory_space_constraint(values, pltpu.HBM)
            for values in (
                velocity.reshape(3, rows, LANES),
                pressure.reshape(rows, LANES),
                pack(fields),
                pack(brownian),
            )
        )
    )
    new_fields, new_velocity = pl.pallas_call(
        write_kernel,
        out_shape=(
            jax.ShapeDtypeStruct((3, count, packed, LANES), jnp.bfloat16),
            jax.ShapeDtypeStruct((3, rows, LANES), jnp.float32),
        ),
        in_specs=[near] * 2,
        out_specs=(pl.BlockSpec(memory_space=pltpu.HBM),) * 2,
        scratch_shapes=[dma((2,))],
        compiler_params=pltpu.CompilerParams(vmem_limit_bytes=VMEM_LIMIT),
    )(*between)
    unpacked = new_fields.reshape(3, count, rows, depth, LANES).transpose(0, 1, 3, 2, 4)
    return (
        unpacked.reshape(3, count, depth, extent),
        new_velocity.reshape(3, 1, extent),
    )


def solution(mesh):
    placed = (
        P(None, ("mesh", "field"), None),
        P(("mesh", "field"), None),
        P(None, "field", "mesh", None),
        P(None, "field", "mesh", None),
    )
    return jax.shard_map(
        functools.partial(body, mesh.shape["mesh"], mesh.shape["field"]),
        mesh=mesh,
        in_specs=placed,
        out_specs=(P(None, "field", "mesh", None), P(None, ("mesh", "field"), None)),
        check_vma=False,
    )
```

```python
import functools

import jax
import jax.numpy as jnp
from jax import lax
from jax.experimental import pallas as pl
from jax.experimental.pallas import tpu as pltpu
from jax.sharding import PartitionSpec as P

NY = 32
NZ = 32
SWEEPS = 4
LANES = 128
CHUNKS = 2
EARLY_CHUNKS = 0
UNROLL = 32
VMEM_LIMIT = 24 * 1024 * 1024

time_step = 0.02
axial_weight = 400.0
transverse_weight = 40.0
weissenberg = 0.5
max_stretch = 50.0
polymer_viscosity = 40.0
noise_scale = (0.02 / 0.5) ** 0.5
diagonal_weight = 1.0 / 0.02 + 2.0 * 400.0 + 4.0 * 40.0
index_table = ((0, 1, 2), (1, 3, 4), (2, 4, 5))
component_pairs = ((0, 0), (0, 1), (0, 2), (1, 1), (1, 2), (2, 2))
diagonal_pairs = (0, 3, 5)


def plane_shifts(x):
    rows = x.shape[0]
    lane = lax.broadcasted_iota(jnp.int32, x.shape, 1)
    row = lax.broadcasted_iota(jnp.int32, x.shape, 0)
    column = lane % NZ
    ahead = pltpu.roll(x, LANES - NZ, 1)
    ahead_next = jnp.where(row == rows - 1, 0.0, pltpu.roll(ahead, rows - 1, 0))
    y_plus = jnp.where(lane >= LANES - NZ, ahead_next, ahead)
    behind = pltpu.roll(x, NZ, 1)
    behind_next = jnp.where(row == 0, 0.0, pltpu.roll(behind, 1, 0))
    y_minus = jnp.where(lane < NZ, behind_next, behind)
    z_plus = jnp.where(column < NZ - 1, pltpu.roll(x, LANES - 1, 1), 0.0)
    z_minus = jnp.where(column > 0, pltpu.roll(x, 1, 1), 0.0)
    return y_plus, y_minus, z_plus, z_minus


def add(left, right):
    if left is None:
        return right
    return left if right is None else left + right


def step_kernel(
    subdomains, groups,
    vel, prs, fld, brn, advanced, out_vel,
    cur, noise, now32, next32, vbuf, pbuf, grads, stress, terms, tx, rx,
    load_sem, flow_sem, send_sem, vel_mates, vel_cross, con_recv, ready,
):
    rows = vel.shape[1]
    count = fld.shape[1]
    packed = fld.shape[2]
    total = subdomains * groups
    block = min(16, packed)
    chunk = count // CHUNKS
    reach = -(-SWEEPS // groups)
    spread = 2 * reach + 1
    sub = lax.axis_index("mesh")
    own = lax.axis_index("field")
    has_prev = sub > 0
    has_next = sub < subdomains - 1

    def inside(shift):
        return (sub + shift >= 0) & (sub + shift < subdomains)

    flow_loads = [
        pltpu.make_async_copy(vel, vbuf.at[own + 1], flow_sem.at[0]),
        pltpu.make_async_copy(prs, pbuf, flow_sem.at[0]),
    ]
    for copy in flow_loads:
        copy.start()

    barrier = pltpu.get_barrier_semaphore()

    def greet(device):
        pl.semaphore_signal(
            barrier, inc=1, device_id=device, device_id_type=pl.DeviceIdType.MESH
        )

    @pl.when(has_next)
    def _():
        greet((sub + 1, 0))

    @pl.when(has_prev)
    def _():
        greet((sub - 1, groups - 1))

    for f in range(groups):
        gathers = own != f
        if f == 0:
            gathers = gathers & jnp.logical_not(has_prev)
        if f == groups - 1:
            gathers = gathers & jnp.logical_not(has_next)

        @pl.when(gathers)
        def _(f=f):
            greet((sub, f))

    for number in range(CHUNKS):
        part = pl.ds(number * chunk, chunk)
        for copy in (
            pltpu.make_async_copy(fld.at[:, part], cur.at[:, part], load_sem.at[number]),
            pltpu.make_async_copy(brn.at[:, part], noise.at[:, part], load_sem.at[number]),
        ):
            copy.start()

    @pl.when(jnp.logical_not(has_prev))
    def _():
        vbuf[0] = jnp.zeros(vbuf.shape[1:], jnp.float32)

    @pl.when(jnp.logical_not(has_next))
    def _():
        vbuf[groups + 1] = jnp.zeros(vbuf.shape[1:], jnp.float32)

    for shift in range(-reach, reach + 1):
        if shift != 0:
            @pl.when(jnp.logical_not(inside(shift)))
            def _(shift=shift):
                rx[pl.ds((reach + shift) * groups, groups)] = jnp.zeros(
                    (groups,) + rx.shape[1:], jnp.float32
                )

    relax = time_step * max_stretch / (2.0 * weissenberg)

    def base_chunk(number):
        both = now32.at[:, pl.ds(0, chunk)]
        pltpu.make_async_copy(both, both, load_sem.at[number]).wait()

        @pl.loop(number * chunk, (number + 1) * chunk, unroll=2)
        def _(n):
            for start in range(0, packed, block):
                at = pl.ds(start, block)
                now = [cur[c, n, at].astype(jnp.float32) for c in range(3)]
                square = now[0] * now[0] + now[1] * now[1] + now[2] * now[2]
                keep = 1.0 - relax * (1.0 / (max_stretch - square))
                for c in range(3):
                    now32[c, n, at] = now[c]
                    next32[c, n, at] = now[c] * keep + noise_scale * noise[c, n, at].astype(jnp.float32)

    for number in range(EARLY_CHUNKS):
        base_chunk(number)

    sends_prev = (own == 0) & has_prev
    sends_next = (own == groups - 1) & has_next
    guided = sends_prev | sends_next

    @pl.when(jnp.logical_not(guided))
    def _():
        pl.semaphore_wait(barrier, groups - 1)

    def admit(helper, device, needed):
        @pl.when((own == helper) & needed)
        def _():
            pl.semaphore_signal(
                ready, inc=1, device_id=(sub, device), device_id_type=pl.DeviceIdType.MESH
            )

    admit(1, 0, has_prev)
    admit(groups - 2, groups - 1, has_next)

    loaded = stress.at[0, pl.ds(0, 4)]
    pltpu.make_async_copy(loaded, loaded, flow_sem.at[0]).wait()

    @pl.when(guided)
    def _():
        pl.semaphore_wait(ready, 1)

    def flow_copy(device, slot, recv):
        return pltpu.make_async_remote_copy(
            src_ref=vbuf.at[own + 1], dst_ref=vbuf.at[slot],
            send_sem=send_sem.at[0], recv_sem=recv,
            device_id=device, device_id_type=pl.DeviceIdType.MESH,
        )

    half = max(1, groups // 2)
    across_first = (own // half + 1) * half

    def to_mates(send):
        for r in range(groups):
            f = (across_first + r) % groups

            @pl.when(f != own)
            def _(f=f):
                send(f).start()

    arrives = vel_mates.at[jnp.where(own == 0, 1, 0)]
    to_mates(lambda f: flow_copy((sub, f), own + 1, arrives))

    @pl.when(sends_prev)
    def _():
        pl.semaphore_wait(barrier, groups)
        for f in sorted(range(groups), key=lambda f: (f % 2, -f)):
            flow_copy((sub - 1, f), groups + 1, vel_cross.at[1]).start()

    @pl.when(sends_next)
    def _():
        pl.semaphore_wait(barrier, groups)
        for f in sorted(range(groups), key=lambda f: (f % 2, f)):
            flow_copy((sub + 1, f), 0, vel_cross.at[0]).start()

    for number in range(EARLY_CHUNKS, CHUNKS):
        base_chunk(number)

    factor = polymer_viscosity / weissenberg

    scale = 0.5 * time_step

    def prepare_fields(q):
        g = [None] * 9
        for a in range(3):
            g[3 * a] = vbuf[q, a] * -scale
            g[3 * a + 1] = grads[q, a]
            g[3 * a + 2] = grads[q, 3 + a]
        at = pl.ds(q, rows, stride=groups)

        @pl.loop(0, count, unroll=UNROLL // 2)
        def _(n):
            now = [now32[c, n, at] for c in range(3)]
            for a in range(3):
                next32[a, n, at] = next32[a, n, at] + (
                    g[3 * a] * now[0] + g[3 * a + 1] * now[1] + g[3 * a + 2] * now[2]
                )

    def plane_fields(q, prepared=False):
        g = [None] * 9
        for a in range(3):
            if prepared:
                g[3 * a] = vbuf[q + 2, a] * scale
                continue
            g[3 * a] = (vbuf[q + 2, a] - vbuf[q, a]) * scale
            g[3 * a + 1] = grads[q, a]
            g[3 * a + 2] = grads[q, 3 + a]
        at = pl.ds(q, rows, stride=groups)

        def one_field(n, acc):
            now = [now32[c, n, at] for c in range(1 if prepared else 3)]
            new = []
            for a in range(3):
                stretch = g[3 * a] * now[0]
                if not prepared:
                    stretch = stretch + g[3 * a + 1] * now[1] + g[3 * a + 2] * now[2]
                value = next32[a, n, at] + stretch
                next32[a, n, at] = value
                new.append(value)
            square = new[0] * new[0] + new[1] * new[1] + new[2] * new[2]
            inverse = 1.0 / (max_stretch - square)
            pulled = [inverse * value for value in new]
            return tuple(
                total_k + pulled[left] * new[right]
                for total_k, (left, right) in zip(acc, component_pairs)
            )

        zero = jnp.zeros((rows, LANES), jnp.float32)
        acc = lax.fori_loop(0, count, one_field, (zero,) * 6, unroll=UNROLL)
        for k in range(6):
            value = acc[k] * (factor * max_stretch / (count * groups))
            stress[q, k] = value - factor / groups if k in diagonal_pairs else value

    across = (
        lax.broadcasted_iota(jnp.int32, (rows, LANES), 0) * (LANES // NZ)
        + lax.broadcasted_iota(jnp.int32, (rows, LANES), 1) // NZ
    )
    solid = jnp.where((across < NY // 4) | (across >= NY - NY // 4), 1.0, 0.0)
    first, last = -reach * groups, groups - 1 + reach * groups
    mine = [jnp.where(own == q, 1.0, 0.0) for q in range(groups)]
    y_plus, y_minus, z_plus, z_minus = plane_shifts(pbuf[...])
    pressure_slopes = (None, y_plus - y_minus, z_plus - z_minus)
    for a in range(3):
        mid = vbuf[own + 1, a]
        y_plus, y_minus, z_plus, z_minus = plane_shifts(mid)
        terms[a] = transverse_weight * ((y_plus + y_minus) + (z_plus + z_minus))
        value = mid * (1.0 / time_step)
        terms[3 + a] = value if a == 0 else value - 0.5 * pressure_slopes[a]

    def fluid(d):
        plane = sub * groups + d
        exists = jnp.where((plane >= 0) & (plane < total), 1.0 / diagonal_weight, 0.0)
        narrow = jnp.where(plane >= total // 2, 1.0, 0.0)
        return exists * (1.0 - narrow * solid)

    def momentum(outputs, lowest=first):
        needs = {SWEEPS: sorted(outputs)}
        for sweep in range(SWEEPS, 1, -1):
            around = {d + e for d in needs[sweep] for e in (-1, 0, 1)}
            needs[sweep - 1] = sorted(
                d for d in around if max(-sweep, lowest - 1) < d < groups + sweep - 1
            )
        scale_of = {}
        source = {}
        start = {}
        for d in sorted({d for ds in needs.values() for d in ds}):
            scale_of[d] = fluid(d)
            if not -1 <= d <= groups:
                continue
            along_y = {}
            along_z = {}
            if 0 <= d < groups:
                for k in range(1, 6):
                    y_plus, y_minus, z_plus, z_minus = plane_shifts(stress[d, k])
                    along_y[k] = y_plus - y_minus
                    along_z[k] = z_plus - z_minus
            for a in range(3):
                slope = None
                beside = 0.0
                for e, sign in ((1, 1.0), (-1, -1.0)):
                    if 0 <= d + e < groups:
                        other = stress[d + e, a]
                        if a == 0:
                            other = other - mine[d + e] * pbuf[...]
                        slope = add(slope, sign * other)
                        beside = beside + mine[d + e]
                if 0 <= d < groups:
                    slope = add(slope, along_y[index_table[a][1]] + along_z[index_table[a][2]])
                value = 0.5 * slope
                begin = (axial_weight * beside) * vbuf[own + 1, a]
                if 0 <= d < groups:
                    value = value + mine[d] * terms[3 + a]
                    begin = begin + mine[d] * terms[a]
                source[d, a] = scale_of[d] * value
                start[d, a] = source[d, a] + scale_of[d] * begin
        pull = {d: value * transverse_weight for d, value in scale_of.items()}
        ratio = axial_weight / transverse_weight
        v = {(d, a): start[d, a] for d in needs[1] for a in range(3)}
        for sweep in range(2, SWEEPS + 1):
            fresh = {}
            for d in needs[sweep]:
                for a in range(3):
                    value = add(v.get((d + 1, a)), v.get((d - 1, a)))
                    if value is not None:
                        value = value * ratio
                    if (d, a) in v:
                        y_plus, y_minus, z_plus, z_minus = plane_shifts(v[d, a])
                        value = add(value, (y_plus + y_minus) + (z_plus + z_minus))
                    fresh[d, a] = add(source.get((d, a)), pull[d] * value)
            v = fresh
        for d in outputs:
            for a in range(3):
                tx[d - first, a] = v[d, a]

    def share(shift, f):
        return pltpu.make_async_remote_copy(
            src_ref=tx.at[(reach + shift) * groups + f],
            dst_ref=rx.at[(reach - shift) * groups + own],
            send_sem=send_sem.at[0], recv_sem=con_recv.at[0],
            device_id=(sub + shift, f), device_id_type=pl.DeviceIdType.MESH,
        )

    def wait_velocity(number, sem):
        planes = vbuf.at[pl.ds(0, number)]
        pltpu.make_async_copy(planes, planes, sem).wait()

    def cross_slopes(planes):
        for q in planes:
            for a in range(3):
                y_plus, y_minus, z_plus, z_minus = plane_shifts(vbuf[q + 1, a])
                grads[q, a] = (y_plus - y_minus) * scale
                grads[q, 3 + a] = (z_plus - z_minus) * scale

    @pl.when(own == 0)
    def _():
        wait_velocity(groups - 1, vel_mates.at[0])

    @pl.when(own != 0)
    def _():
        wait_velocity(groups - 2, vel_mates.at[0])

    @pl.when((own != 0) & (own < half))
    def _():
        wait_velocity(1, vel_mates.at[1])

    @pl.when(own < half)
    def _():
        cross_slopes(range(groups))

    @pl.when(own >= half)
    def _():
        cross_slopes(range(1, groups))

    for q in reversed(range(2, groups - 1)):
        plane_fields(q)

    @pl.when(own >= half)
    def _():
        wait_velocity(1, vel_mates.at[1])
        cross_slopes(range(1))

    plane_fields(1)

    @pl.when(has_prev)
    def _():
        pltpu.make_async_copy(vbuf.at[0], vbuf.at[0], vel_cross.at[0]).wait()

    plane_fields(0)

    early = groups - 1 - SWEEPS - first

    @pl.when(has_prev)
    def _():
        momentum([first])
        share(-reach, 0).start()
        momentum(range(first + 1, first + early))
        for r in range(groups):
            f = (across_first + r) % groups

            @pl.when((f > 0) & (f < early))
            def _(f=f):
                share(-reach, f).start()

    prepare_fields(groups - 1)

    @pl.when(has_next)
    def _():
        pltpu.make_async_copy(vbuf.at[0], vbuf.at[0], vel_cross.at[1]).wait()

    plane_fields(groups - 1, True)
    def share_next():
        for r in sorted(range(groups), key=lambda r: (r // half, -r)):
            share(reach, (across_first + r) % groups).start()

    @pl.when(has_prev)
    def _():
        @pl.when(has_next)
        def _():
            momentum(range(groups, last + 1))
            share_next()

        momentum(range(first + early, groups))
        for f in range(early, groups):
            share(-reach, f).start()
        to_mates(lambda f: share(0, f))

    @pl.when(jnp.logical_not(has_prev))
    def _():
        momentum(range(0, groups), 0)
        to_mates(lambda f: share(0, f))

        @pl.when(has_next)
        def _():
            momentum(range(groups, last + 1), 0)
            share_next()

    here = reach * groups + own
    rx[here] = tx[here]

    @pl.loop(0, count, unroll=2)
    def _(n):
        for c in range(3):
            for start in range(0, packed, block):
                at = pl.ds(start, block)
                advanced[c, n, at] = next32[c, n, at].astype(jnp.bfloat16)

    partners = groups - 1
    for shift in range(-reach, reach + 1):
        if shift != 0:
            partners = partners + jnp.where(inside(shift), groups, 0)
    sent_flow = groups - 1 + jnp.where(sends_prev, groups, 0) + jnp.where(sends_next, groups, 0)

    def wait_planes(number, options, sem):
        for option in options:
            @pl.when(number == option)
            def _(option=option):
                planes = now32.at[:, pl.ds(0, option), pl.ds(0, rows)]
                pltpu.make_async_copy(planes, planes, sem).wait()

    wait_planes(partners, [groups - 1 + k * groups for k in range(spread)], con_recv.at[0])
    for a in range(3):
        value = rx[0, a]
        for k in range(1, spread * groups):
            value = value + rx[k, a]
        out_vel[a] = value
    wait_planes(
        partners + sent_flow,
        [2 * (groups - 1) + k * groups for k in range(spread + 1)],
        send_sem.at[0],
    )


def write_kernel(advanced, velocity, out_fields, out_vel, out_sem):
    copies = [
        pltpu.make_async_copy(advanced, out_fields, out_sem.at[0]),
        pltpu.make_async_copy(velocity, out_vel, out_sem.at[1]),
    ]
    for copy in copies:
        copy.start()
    for copy in copies:
        copy.wait()


def body(subdomains, groups, velocity, pressure, fields, brownian):
    extent = velocity.shape[2]
    count, depth = fields.shape[1], fields.shape[2]
    rows = extent // LANES
    packed = rows * depth
    slots = (2 * (-(-SWEEPS // groups)) + 1) * groups

    def pack(values):
        split = values.reshape(3, count, depth, rows, LANES)
        return split.transpose(0, 1, 3, 2, 4).reshape(3, count, packed, LANES)

    dma = pltpu.SemaphoreType.DMA
    near = pl.BlockSpec(memory_space=pltpu.VMEM)
    between = pl.pallas_call(
        functools.partial(step_kernel, subdomains, groups),
        out_shape=(
            pltpu.VMEM((3, count, packed, LANES), jnp.bfloat16),
            pltpu.VMEM((3, rows, LANES), jnp.float32),
        ),
        in_specs=[pl.BlockSpec(memory_space=pltpu.HBM)] * 4,
        out_specs=(near,) * 2,
        scratch_shapes=[
            pltpu.VMEM((3, count, packed, LANES), jnp.bfloat16),
            pltpu.VMEM((3, count, packed, LANES), jnp.bfloat16),
            pltpu.VMEM((3, count, packed, LANES), jnp.float32),
            pltpu.VMEM((3, count, packed, LANES), jnp.float32),
            pltpu.VMEM((groups + 2, 3, rows, LANES), jnp.float32),
            pltpu.VMEM((rows, LANES), jnp.float32),
            pltpu.VMEM((groups, 6, rows, LANES), jnp.float32),
            pltpu.VMEM((groups, 6, rows, LANES), jnp.float32),
            pltpu.VMEM((6, rows, LANES), jnp.float32),
            pltpu.VMEM((slots, 3, rows, LANES), jnp.float32),
            pltpu.VMEM((slots, 3, rows, LANES), jnp.float32),
            dma((CHUNKS,)),
            dma((1,)),
            dma((1,)),
            dma((2,)),
            dma((2,)),
            dma((1,)),
            pltpu.SemaphoreType.REGULAR,
        ],
        compiler_params=pltpu.CompilerParams(
            collective_id=0, has_side_effects=True, vmem_limit_bytes=VMEM_LIMIT
        ),
    )(
        *(
            pltpu.with_memory_space_constraint(values, pltpu.HBM)
            for values in (
                velocity.reshape(3, rows, LANES),
                pressure.reshape(rows, LANES),
                pack(fields),
                pack(brownian),
            )
        )
    )
    new_fields, new_velocity = pl.pallas_call(
        write_kernel,
        out_shape=(
            jax.ShapeDtypeStruct((3, count, packed, LANES), jnp.bfloat16),
            jax.ShapeDtypeStruct((3, rows, LANES), jnp.float32),
        ),
        in_specs=[near] * 2,
        out_specs=(pl.BlockSpec(memory_space=pltpu.HBM),) * 2,
        scratch_shapes=[dma((2,))],
        compiler_params=pltpu.CompilerParams(vmem_limit_bytes=VMEM_LIMIT),
    )(*between)
    unpacked = new_fields.reshape(3, count, rows, depth, LANES).transpose(0, 1, 3, 2, 4)
    return (
        unpacked.reshape(3, count, depth, extent),
        new_velocity.reshape(3, 1, extent),
    )


def solution(mesh):
    placed = (
        P(None, ("mesh", "field"), None),
        P(("mesh", "field"), None),
        P(None, "field", "mesh", None),
        P(None, "field", "mesh", None),
    )
    return jax.shard_map(
        functools.partial(body, mesh.shape["mesh"], mesh.shape["field"]),
        mesh=mesh,
        in_specs=placed,
        out_specs=(P(None, "field", "mesh", None), P(None, ("mesh", "field"), None)),
        check_vma=False,
    )
```
